256 devices in a mesh: slab: 128 (over z, x, y), head: 2 (over core).
Axes of the slice: x: 4, y: 4, z: 8, core: 2. Of those that a mesh axis runs over, the one named last changes fastest.
Arguments:
- directions: bfloat16 [2, 32768, 5120], P(None, 'slab', 'head'), may hold values from -0.59765625 to 0.59765625
- magnitudes: float32 [4, 40, 32768], P(None, 'head', 'slab'), may hold values from 4 to 24
- outlier_rows: bfloat16 [16384, 4, 5120], P('slab', None, 'head'), may hold values from -6 to 6
- outlier_counts: int32 [128], P('slab'), may hold values from 64 to 128
- destinations: int32 [16384, 1], P('slab'), may hold values from 0 to 127; in each aligned block of 128 rows (0 to 127, 128 to 255, ...) at most 2 rows name the same one
- retention_order: int32 [128, 256], P('slab'), may hold values from 0 to 255, each once within a row
Outputs:
- restored: bfloat16 [4, 32768, 5120], P(None, 'slab', 'head')
The draws below stay inside these ranges and needn't reach their ends.
Inputs may be any that keep to these rules, and one draw needn't show every extreme that they name: `outlier_counts`: at least 64 rows of each slab are live. `destinations`: among the 128 rows of one slab at most 2 name the same destination slab. `retention_order`: each slab's row is a permutation of its token positions.
All inputs are finite; a program needn't handle non-finite values.
Results may differ from the reference program's by a relative error of at most 0.0013.
Values may be sent and summed in bfloat16 or wider, within the bound.
No kernel may reach another device: no remote copies, remote signals or barrier semaphores. Data moves between devices by JAX's collectives and lax.ppermute only.
A program may use at most 128 MiB of HBM per device.

```python
import math
import jax
import jax.numpy as jnp
import numpy as np

HEADS = 40
HEAD_DIM = 128
FEAT = 5120
TOK_DEV = 256
OUT_DEV = 128
PAIR_CAP = 2
TOKENS = 32768
SLOTS = 16384
N_SLAB = 128


def with_ends(entries, rng, smallest, top_value):
    extent = entries.shape
    place = [jax.random.randint(jax.random.fold_in(rng, axis), (), 0, extent[axis]) for axis in range(len(extent))]
    entries = entries.at[tuple(place)].set(smallest)
    longest = extent.index(max(extent))
    place[longest] = (place[longest] + 1) % extent[longest]
    return entries.at[tuple(place)].set(top_value)


def levels(stream_key, extent, shards, smallest, largest):
    level, own = 1.0, jax.random.fold_in(stream_key, 6)
    for dim, parts in shards:
        steps = jnp.exp(jax.random.uniform(jax.random.fold_in(own, dim), (parts,), jnp.float32, smallest / len(shards), largest / len(shards)))
        level = level * jnp.repeat(steps, extent[dim] // parts).reshape([-1 if axis == dim else 1 for axis in range(len(extent))])
    return level


def assign_block(rng, own, number, rows, number_of, top, most, skew):
    sequence = jax.random.permutation(rng, number_of)
    packed, usual = portions_of(number_of, rows * top, most, skew, True), portions_of(number_of, rows * top, most, skew, False)
    places = jnp.arange(number_of)

    def named(sizes, rotation):
        used = int((sizes > 0).sum())
        fixed = max(1, used // 4)
        moved = fixed + (places - fixed + rotation * (used - fixed)) % max(1, number_of - fixed)
        return jnp.zeros((number_of,), jnp.int32).at[sequence[jnp.where(places < fixed, places, moved)]].set(jnp.asarray(sizes, jnp.int32))

    sizes = jnp.where(number % 4 == 0, named(packed, number // 4), named(usual, number - number // 4 - 1))
    mixed = jax.random.permutation(jax.random.fold_in(own, 3), number_of)
    giver, sink = mixed[0:number_of // 2 * 2:2], mixed[1:number_of // 2 * 2:2]
    room = jnp.minimum(sizes[giver] - 1, most - sizes[sink]) // 2
    room = jnp.where((giver == sequence[0]) | (sink == sequence[0]) | (sizes[sink] == 0), 0, jnp.maximum(room, 0))
    moved = jax.random.randint(jax.random.fold_in(own, 4), (number_of // 2,), 0, 1 << 20) % (room + 1)
    sizes = sizes.at[giver].add(-moved).at[sink].add(moved)
    items = jnp.searchsorted(jnp.cumsum(sizes), jnp.arange(rows * top), side="right").astype(jnp.int32)
    listing = items.reshape(top, rows).T
    listing = listing[jax.random.permutation(jax.random.fold_in(own, 1), rows)]
    rotation = jax.random.randint(jax.random.fold_in(own, 2), (rows, 1), 0, top)
    return jnp.take_along_axis(listing, (jnp.arange(top)[None, :] + rotation) % top, axis=1)


def portions_of(amount, total, limit, lean, full):
    weights = [(1 << 20) // math.isqrt(standing ** lean) + 1 for standing in range(1, amount + 1)]
    largest = limit if full else min(limit, max(-(-total // amount), total * weights[0] // sum(weights)))
    least = 1 if total - largest >= amount - 1 else 0
    given, spare = [largest] + [least] * (amount - 1), total - largest - least * (amount - 1)
    while spare > 0:
        free = [i for i in range(1, amount) if given[i] < largest] or [i for i in range(1, amount) if given[i] < limit]
        whole, remaining = sum([weights[i] for i in free]), spare
        for i in free:
            extra = min(limit - given[i], max(1, remaining * weights[i] // whole), spare)
            given[i] = given[i] + extra
            spare = spare - extra
    return np.array(given)


def gaussian(key, extent, spread, bound, pieces=(), kind=jnp.bfloat16):
    entries = jax.random.normal(key, extent, jnp.float32) * spread
    if len(pieces) > 0:
        entries = levels(key, extent, pieces, -0.22, 0.18) * entries
    return jnp.clip(entries, min=-bound, max=bound).astype(kind)


def setup_inputs(seed: int = 0) -> dict:
    streams_of = jax.random.split(jax.random.key(seed), 7)
    directions = gaussian(streams_of[0], (2, TOKENS, FEAT), 0.088, 0.59765625, ((1, 128), (2, 2)))
    magnitudes = jnp.clip(jnp.exp(math.log(24.0) - 1.7917595 * jax.random.uniform(streams_of[1], (4, HEADS, TOKENS), jnp.float32) ** levels(streams_of[1], (4, HEADS, TOKENS), ((1, 2), (2, 128)), -0.2, 0.2)), 4.0, 24.0)
    outlier_rows = gaussian(streams_of[2], (SLOTS, 4, FEAT), 1.0, 6.0, ((0, 128), (2, 2)))
    outlier_counts = with_ends(jax.random.randint(streams_of[3], (N_SLAB,), OUT_DEV // 2, OUT_DEV + 1), jax.random.fold_in(streams_of[3], 1), OUT_DEV // 2, OUT_DEV).astype(jnp.int32)
    destinations_keys = jax.random.split(jax.random.fold_in(streams_of[4], 1), SLOTS // OUT_DEV)
    destinations_turns = jax.random.permutation(jax.random.fold_in(streams_of[4], 3), SLOTS // OUT_DEV)
    destinations = jax.vmap(lambda own, number: assign_block(jax.random.fold_in(streams_of[4], 2), own, number, OUT_DEV, N_SLAB, 1, PAIR_CAP, 2))(destinations_keys, destinations_turns).reshape((SLOTS, 1))
    retention_order = jax.vmap(lambda own: jax.random.permutation(own, TOK_DEV))(jax.random.split(streams_of[5], N_SLAB)).reshape((N_SLAB, TOK_DEV)).astype(jnp.int32)
    return dict(directions=directions, magnitudes=magnitudes, outlier_rows=outlier_rows, outlier_counts=outlier_counts, destinations=destinations, retention_order=retention_order)


def reference(directions, magnitudes, outlier_rows, outlier_counts, destinations, retention_order):
    token_dirs = jnp.roll(directions, -1, axis=1)
    token_mags = jnp.roll(magnitudes, -1, axis=2)
    target = destinations[:, 0].reshape(N_SLAB, OUT_DEV).astype(jnp.int32)
    active = jnp.arange(OUT_DEV, dtype=jnp.int32)[None, :] < outlier_counts[:, None]
    chosen = ((target[:, :, None] == jnp.arange(N_SLAB, dtype=jnp.int32)[None, None, :]) & active[:, :, None]).astype(jnp.int32)
    pair_counts = jnp.sum(chosen, axis=1)
    offsets = jnp.cumsum(pair_counts, axis=0) - pair_counts
    within = jnp.sum(chosen * (jnp.cumsum(chosen, axis=1) - 1), axis=2)
    arrival = jnp.sum(chosen * offsets[:, None, :], axis=2) + within
    position = retention_order[target, jnp.clip(arrival, 0, TOK_DEV - 1)]
    landing = jnp.where(active, target * TOK_DEV + position, TOKENS).reshape(-1).astype(jnp.int32)
    outputs = []
    for index in range(4):
        factor = jnp.transpose(token_mags[index])[:, :, None]
        scaled = factor * token_dirs[index % 2].reshape(TOKENS, HEADS, HEAD_DIM).astype(jnp.float32)
        scaled = scaled.reshape(TOKENS, FEAT).astype(jnp.bfloat16)
        outputs.append(scaled.at[landing].set(outlier_rows[:, index, :], mode="drop"))
    return jnp.stack(outputs)
```

```python
import jax
import jax.numpy as jnp
from jax import lax
from jax.experimental import pallas as pl
from jax.experimental.pallas import tpu as pltpu
from jax.sharding import Mesh
from jax.sharding import PartitionSpec as P

SLAB = ("slab_0", "slab_1", "slab_2")
EMPTY = 2.0**127


def pack_kernel(pair_cap, dest_ref, count_ref, rows_ref, out_ref, seen, sem):
    slabs = seen.shape[0]
    slots = out_ref.shape[0]
    step = 16

    def fill(i, carry):
        out_ref[pl.ds(i * step, step)] = jnp.full((step,) + out_ref.shape[1:], EMPTY, out_ref.dtype)
        return carry

    lax.fori_loop(0, slots // step, fill, 0)

    def clear(i, carry):
        seen[i] = 0
        return carry

    lax.fori_loop(0, slabs, clear, 0, unroll=8)
    live = count_ref[0]

    def send(r, carry):
        d = dest_ref[r]
        j = seen[d]
        seen[d] = j + 1
        pltpu.make_async_copy(rows_ref.at[r], out_ref.at[d * pair_cap + j], sem).start()
        return carry

    lax.fori_loop(0, live, send, 0)

    def finish(r, carry):
        pltpu.make_async_copy(rows_ref.at[0], out_ref.at[0], sem).wait()
        return carry

    lax.fori_loop(0, live, finish, 0)


def pack(outlier_rows, destinations, outlier_counts, slab_count, pair_cap):
    row_slots, kinds, features = outlier_rows.shape
    smem = pl.BlockSpec(memory_space=pltpu.SMEM)
    return pl.pallas_call(
        lambda *refs: pack_kernel(pair_cap, *refs),
        name="pack",
        in_specs=[smem, smem, pl.BlockSpec(memory_space=pl.ANY)],
        out_specs=pl.BlockSpec(memory_space=pltpu.VMEM),
        out_shape=jax.ShapeDtypeStruct((slab_count * pair_cap, kinds, features), outlier_rows.dtype),
        scratch_shapes=[pltpu.SMEM((slab_count,), jnp.int32), pltpu.SemaphoreType.DMA],
        cost_estimate=pl.CostEstimate(
            flops=0, bytes_accessed=3 * row_slots * kinds * features * 2, transcendentals=0
        ),
    )(destinations[:, 0], outlier_counts, outlier_rows)


def scale_kernel(dirs_ref, mags_ref, out_ref):
    tokens, width = dirs_ref.shape[1], dirs_ref.shape[2]
    head_size = 128
    heads = mags_ref.shape[1]
    col0 = pl.program_id(0) * (width // head_size)
    for v in range(2):
        ahead = pltpu.roll(dirs_ref[v].astype(jnp.float32), tokens - 1, 0)
        for k in (v, v + 2):
            for c in range(width // head_size):
                out_ref[k, :, c * head_size : (c + 1) * head_size] = (
                    mags_ref[k, c] * ahead[:, c * head_size : (c + 1) * head_size]
                ).astype(out_ref.dtype)


def scale(directions, factors):
    _, tokens, features = directions.shape
    heads_per = 2
    width = heads_per * 128
    return pl.pallas_call(
        scale_kernel,
        name="scale",
        grid=(features // width,),
        in_specs=[
            pl.BlockSpec((2, tokens, width), lambda i: (0, 0, i)),
            pl.BlockSpec((4, heads_per, tokens, 1), lambda i: (0, i, 0, 0)),
        ],
        out_specs=pl.BlockSpec((4, tokens, width), lambda i: (0, 0, i)),
        out_shape=jax.ShapeDtypeStruct((4, tokens, features), directions.dtype),
        cost_estimate=pl.CostEstimate(
            flops=20 * tokens * features, bytes_accessed=12 * tokens * features, transcendentals=0
        ),
    )(directions, factors)


def place_kernel(arrived_ref, rank_ref, edge_ref, scaled_ref, out_ref, placer, covered):
    slots, kinds, width = arrived_ref.shape
    tokens = out_ref.shape[1]
    total = slots * kinds
    rows = arrived_ref[...].reshape(total, width)

    @pl.when(pl.program_id(0) == 0)
    def _():
        first = rows[:, 0:128].astype(jnp.float32)
        kind_of = lax.broadcasted_iota(jnp.int32, (total, 128), 0) % kinds
        full = jnp.where((kind_of == 0) & (first < EMPTY), 1.0, 0.0).astype(jnp.bfloat16)
        source = lax.broadcasted_iota(jnp.int32, (total, total), 0) // kinds
        target = lax.broadcasted_iota(jnp.int32, (total, total), 1) // kinds
        earlier = jnp.where(source < target, 1.0, 0.0).astype(jnp.bfloat16)
        same = jnp.where(source == target, 1.0, 0.0).astype(jnp.bfloat16)
        over = (((0,), (0,)), ((), ()))
        arrival = lax.dot_general(full, earlier, over, preferred_element_type=jnp.float32)[0:1]
        filled = lax.dot_general(full, same, over, preferred_element_type=jnp.float32)[0:1]
        arrival = jnp.where(filled > 0.5, arrival, -1.0).astype(jnp.int32)
        here = rank_ref[...] == arrival
        kind = lax.broadcasted_iota(jnp.int32, (tokens, total), 1) % kinds
        for k in range(kinds):
            placer[k] = jnp.where(here & (kind == k), 1.0, 0.0).astype(jnp.bfloat16)
        count = jnp.sum(full[:, 0:1].astype(jnp.float32)).astype(jnp.int32)
        covered[...] = jnp.where(rank_ref[...] < count, 1, 0) * jnp.ones((1, 128), jnp.int32)

    last = lax.broadcasted_iota(jnp.int32, (tokens, width), 0) == tokens - 1
    taken = jnp.concatenate([covered[...]] * (width // 128), axis=1) > 0
    for k in range(kinds):
        inserted = jnp.dot(placer[k], rows, preferred_element_type=jnp.float32)
        own = jnp.where(last, edge_ref[k : k + 1], scaled_ref[k].astype(jnp.float32))
        out_ref[k] = jnp.where(taken, inserted, own).astype(out_ref.dtype)


def place(arrived, rank, edge, scaled):
    slots, kinds, features = arrived.shape
    _, tokens, _ = scaled.shape
    width = 256
    return pl.pallas_call(
        place_kernel,
        name="place",
        grid=(features // width,),
        in_specs=[
            pl.BlockSpec((slots, kinds, width), lambda i: (0, 0, i)),
            pl.BlockSpec((tokens, 1), lambda i: (0, 0)),
            pl.BlockSpec((8, width), lambda i: (0, i)),
            pl.BlockSpec((kinds, tokens, width), lambda i: (0, 0, i)),
        ],
        out_specs=pl.BlockSpec((kinds, tokens, width), lambda i: (0, 0, i)),
        out_shape=jax.ShapeDtypeStruct(scaled.shape, scaled.dtype),
        scratch_shapes=[
            pltpu.VMEM((kinds, tokens, slots * kinds), jnp.bfloat16),
            pltpu.VMEM((tokens, 128), jnp.int32),
        ],
        cost_estimate=pl.CostEstimate(
            flops=2 * kinds * tokens * slots * kinds * features,
            bytes_accessed=2 * (slots * kinds + 2 * kinds * tokens) * features,
            transcendentals=0,
        ),
    )(arrived, rank, edge, scaled)


def passed_back(block, axis):
    devices = lax.axis_size(axis)
    return lax.ppermute(block, axis, [((i + 1) % devices, i) for i in range(devices)])


def per_device(directions, magnitudes, outlier_rows, outlier_counts, destinations, retention_order):
    slab_count = lax.axis_size(SLAB)
    tokens, features = directions.shape[1], directions.shape[2]
    heads = magnitudes.shape[1]
    head_size = features // heads
    pair_cap = max(2, tokens // slab_count)

    edge = jnp.concatenate(
        [directions[:, 0, :].astype(jnp.float32).reshape(-1), magnitudes[:, :, 0].reshape(-1)]
    )
    edge = passed_back(edge, SLAB)
    packed = pack(outlier_rows, destinations, outlier_counts, slab_count, pair_cap)
    arrived = lax.all_to_all(packed, SLAB, split_axis=0, concat_axis=0, tiled=True)

    edge_dirs = edge[: 2 * features].reshape(1, 2, heads, head_size)
    edge_mags = edge[2 * features :].reshape(2, 2, heads, 1)
    edge_row = (edge_mags * edge_dirs).astype(jnp.bfloat16).astype(jnp.float32).reshape(4, features)
    edge_row = jnp.concatenate([edge_row, edge_row], axis=0)
    factors = jnp.roll(magnitudes, -1, axis=2)[:, :, :, None]
    scaled = scale(directions, factors)
    sequence = retention_order[0]
    positions = jnp.arange(tokens, dtype=jnp.int32)
    rank = jnp.sum(
        jnp.where(sequence[None, :] == positions[:, None], positions[None, :], 0), axis=1, keepdims=True
    )
    return place(arrived, rank, edge_row, scaled)


def solution(mesh):
    finer = Mesh(
        mesh.devices.reshape(8, 4, 4, mesh.shape["head"]), ("slab_0", "slab_1", "slab_2", "head")
    )
    placed = (
        P(None, SLAB, "head"),
        P(None, "head", SLAB),
        P(SLAB, None, "head"),
        P(SLAB),
        P(SLAB, None),
        P(SLAB, None),
    )
    return jax.shard_map(
        per_device, mesh=finer, in_specs=placed, out_specs=P(None, SLAB, "head"), check_vma=False
    )
```

```python
import jax
import jax.numpy as jnp
from jax import lax
from jax.experimental import pallas as pl
from jax.experimental.pallas import tpu as pltpu
from jax.sharding import Mesh
from jax.sharding import PartitionSpec as P

SLAB = ("slab_0", "slab_1", "slab_2")
EMPTY = 2.0**127
WIDTH = 512
DEPTH = 2


def pack_kernel(pair_cap, dest_ref, count_ref, rows_ref, out_ref, held, blank, seen, slot, in_sem, out_sem):
    slabs = seen.shape[0]
    parts = in_sem.shape[0]
    size = held.shape[0] // parts

    def fetch(p):
        part = pl.ds(p * size, size)
        return pltpu.make_async_copy(rows_ref.at[part], held.at[part], in_sem.at[p])

    for p in range(parts):
        fetch(p).start()
    blank[...] = jnp.full(blank.shape, EMPTY, blank.dtype)

    def clear(i, carry):
        seen[i] = 0
        return carry

    lax.fori_loop(0, slabs, clear, 0, unroll=8)
    live = count_ref[0]

    def number(r, carry):
        d = dest_ref[r]
        j = seen[d]
        seen[d] = j + 1
        slot[r] = d * pair_cap + j
        return carry

    lax.fori_loop(0, live, number, 0)

    def leave(d, carry):
        for j in range(pair_cap):

            @pl.when(seen[d] <= j)
            def _():
                pltpu.make_async_copy(blank.at[0], out_ref.at[d * pair_cap + j], out_sem).start()

        return carry

    lax.fori_loop(0, slabs, leave, 0, unroll=4)
    for p in range(parts):
        fetch(p).wait()

    def send(r, carry):
        pltpu.make_async_copy(held.at[r], out_ref.at[slot[r]], out_sem).start()
        return carry

    lax.fori_loop(0, live, send, 0)
    pltpu.make_async_copy(out_ref, out_ref, out_sem).wait()


def pack(outlier_rows, destinations, outlier_counts, slab_count, pair_cap):
    row_slots, kinds, features = outlier_rows.shape
    smem = pl.BlockSpec(memory_space=pltpu.SMEM)
    anywhere = pl.BlockSpec(memory_space=pl.ANY)
    return pl.pallas_call(
        lambda *refs: pack_kernel(pair_cap, *refs),
        name="pack",
        in_specs=[smem, smem, anywhere],
        out_specs=anywhere,
        out_shape=jax.ShapeDtypeStruct((slab_count * pair_cap, kinds, features), outlier_rows.dtype),
        scratch_shapes=[
            pltpu.VMEM(outlier_rows.shape, outlier_rows.dtype),
            pltpu.VMEM((1, kinds, features), outlier_rows.dtype),
            pltpu.SMEM((slab_count,), jnp.int32),
            pltpu.SMEM((row_slots,), jnp.int32),
            pltpu.SemaphoreType.DMA((4,)),
            pltpu.SemaphoreType.DMA,
        ],
        cost_estimate=pl.CostEstimate(
            flops=0, bytes_accessed=3 * row_slots * kinds * features * 2, transcendentals=0
        ),
    )(destinations[:, 0], outlier_counts, outlier_rows)


def shift_kernel(dirs_ref, edge_ref, out_ref):
    tokens, width = dirs_ref.shape[1], dirs_ref.shape[2]
    last = lax.broadcasted_iota(jnp.int32, (tokens, width), 0) == tokens - 1
    for v in range(2):
        ahead = pltpu.roll(dirs_ref[v].astype(jnp.float32), tokens - 1, 0)
        out_ref[v] = jnp.where(last, edge_ref[v : v + 1], ahead).astype(out_ref.dtype)


def shift(directions, edge):
    _, tokens, features = directions.shape
    width = 256
    return pl.pallas_call(
        shift_kernel,
        name="shift",
        compiler_params=pltpu.CompilerParams(vmem_limit_bytes=16 * 2**20),
        grid=(features // width,),
        in_specs=[
            pl.BlockSpec((2, tokens, width), lambda i: (0, 0, i)),
            pl.BlockSpec((2, width), lambda i: (0, i)),
        ],
        out_specs=pl.BlockSpec((2, tokens, width), lambda i: (0, 0, i)),
        out_shape=jax.ShapeDtypeStruct(directions.shape, directions.dtype),
        cost_estimate=pl.CostEstimate(
            flops=20 * tokens * features, bytes_accessed=8 * tokens * features, transcendentals=0
        ),
    )(directions, edge)


def place_kernel(arrived, rank, dirs, mags, out, a_buf, r_buf, d_buf, m_buf, o_buf, placer, covered, wide, a_sem, r_sem, d_sem, m_sem, o_sem):
    blocks, slots, kinds, width = a_buf.shape
    tokens = o_buf.shape[2]
    lanes = 128
    chunks = slots // lanes
    heads = width // lanes

    def columns(i):
        return pl.ds(pl.multiple_of(i * width, lanes), width)

    def a_copy(i):
        return pltpu.make_async_copy(arrived.at[:, :, columns(i)], a_buf.at[i], a_sem.at[i])

    def d_copy(i):
        return pltpu.make_async_copy(dirs.at[:, :, columns(i)], d_buf.at[i], d_sem.at[i])

    def o_copy(i):
        return pltpu.make_async_copy(o_buf.at[i], out.at[:, :, columns(i)], o_sem.at[i])

    r_copy = pltpu.make_async_copy(rank, r_buf, r_sem)
    m_copy = pltpu.make_async_copy(mags, m_buf, m_sem)
    a_copy(0).start()
    r_copy.start()
    m_copy.start()
    d_copy(0).start()
    for i in range(1, DEPTH):
        a_copy(i).start()
        d_copy(i).start()

    r_copy.wait()
    m_copy.wait()

    def block(i, carry):
        @pl.when(i + DEPTH < blocks)
        def _():
            a_copy(i + DEPTH).start()
            d_copy(i + DEPTH).start()

        a_copy(i).wait()
        for c in range(heads):
            wide[c] = (
                a_buf[i, :, :, c * lanes : (c + 1) * lanes]
                .reshape(slots * kinds, lanes)
                .astype(jnp.float32)
            )

        @pl.when(i == 0)
        def _():
            first = wide[0, pl.ds(0, slots, stride=kinds), :]
            full = jnp.where(first < EMPTY, 1.0, 0.0).astype(jnp.bfloat16)
            corner = jnp.where(lax.broadcasted_iota(jnp.int32, (8, lanes), 1) == 0, 1.0, 0.0)
            corner = corner.astype(jnp.bfloat16)
            chunk = lax.broadcasted_iota(jnp.int32, (chunks, lanes), 0)
            over = (((1,), (1,)), ((), ()))
            filled = jnp.zeros((chunks, lanes), jnp.float32)
            for c in range(chunks):
                flags = lax.dot_general(
                    corner, full[c * lanes : (c + 1) * lanes], over, preferred_element_type=jnp.float32
                )
                filled = jnp.where(chunk == c, flags[0:1], filled)
            ones = filled.astype(jnp.bfloat16)
            source = lax.broadcasted_iota(jnp.int32, (lanes, lanes), 0)
            target = lax.broadcasted_iota(jnp.int32, (lanes, lanes), 1)
            tri = jnp.where(source < target, 1.0, 0.0).astype(jnp.bfloat16)
            inside = jnp.dot(ones, tri, preferred_element_type=jnp.float32)
            sums = jnp.dot(ones, jnp.ones((lanes, lanes), jnp.bfloat16), preferred_element_type=jnp.float32)
            ahead = jnp.zeros_like(sums)
            run = jnp.zeros((1, lanes), jnp.float32)
            for c in range(chunks):
                ahead = jnp.where(chunk == c, run, ahead)
                run = run + sums[c : c + 1]
            arrival = jnp.where(filled > 0.5, inside + ahead, -1.0).astype(jnp.int32)
            place_of = r_buf[...]
            covered[...] = jnp.where(place_of < run.astype(jnp.int32), 1, 0)
            for c in range(chunks):
                placer[:, c * lanes : (c + 1) * lanes] = jnp.where(
                    place_of == arrival[c : c + 1], 1.0, 0.0
                ).astype(jnp.bfloat16)

        d_copy(i).wait()
        factors = m_buf[i]
        own_dirs = [d_buf[i, v].astype(jnp.float32) for v in range(2)]
        taken = covered[...] > 0
        for k in range(kinds):
            rows = jnp.concatenate(
                [wide[c, pl.ds(k, slots, stride=kinds), :] for c in range(heads)], axis=1
            ).astype(jnp.bfloat16)
            inserted = jnp.dot(placer[...], rows, preferred_element_type=jnp.float32)
            for c in range(heads):
                part = slice(c * lanes, (c + 1) * lanes)
                own = factors[:, k * heads + c : k * heads + c + 1] * own_dirs[k % 2][:, part]
                o_buf[i, k, :, part] = jnp.where(taken, inserted[:, part], own).astype(o_buf.dtype)
        o_copy(i).start()
        return carry

    lax.fori_loop(0, blocks, block, 0)
    for i in range(blocks):
        o_copy(i).wait()


def place(arrived, rank, dirs, mags):
    slots, kinds, features = arrived.shape
    _, tokens, _ = dirs.shape
    width = WIDTH
    blocks = features // width
    anywhere = pl.BlockSpec(memory_space=pl.ANY)
    return pl.pallas_call(
        place_kernel,
        name="place",
        in_specs=[anywhere] * 4,
        out_specs=anywhere,
        out_shape=jax.ShapeDtypeStruct((kinds, tokens, features), arrived.dtype),
        scratch_shapes=[
            pltpu.VMEM((blocks, slots, kinds, width), arrived.dtype),
            pltpu.VMEM(rank.shape, rank.dtype),
            pltpu.VMEM((blocks, 2, tokens, width), dirs.dtype),
            pltpu.VMEM(mags.shape, mags.dtype),
            pltpu.VMEM((blocks, kinds, tokens, width), arrived.dtype),
            pltpu.VMEM((tokens, slots), jnp.bfloat16),
            pltpu.VMEM((tokens, 128), jnp.int32),
            pltpu.VMEM((width // 128, slots * kinds, 128), jnp.float32),
            pltpu.SemaphoreType.DMA((blocks,)),
            pltpu.SemaphoreType.DMA,
            pltpu.SemaphoreType.DMA((blocks,)),
            pltpu.SemaphoreType.DMA,
            pltpu.SemaphoreType.DMA((blocks,)),
        ],
        cost_estimate=pl.CostEstimate(
            flops=2 * kinds * tokens * slots * features,
            bytes_accessed=2 * (slots * kinds + 2 * tokens + kinds * tokens) * features,
            transcendentals=0,
        ),
    )(arrived, rank, dirs, mags)


def passed_back(block, axis):
    devices = lax.axis_size(axis)
    return lax.ppermute(block, axis, [((i + 1) % devices, i) for i in range(devices)])


def per_device(directions, magnitudes, outlier_rows, outlier_counts, destinations, retention_order):
    slab_count = lax.axis_size(SLAB)
    tokens, features = directions.shape[1], directions.shape[2]
    heads = magnitudes.shape[1]
    head_size = features // heads
    pair_cap = max(2, tokens // slab_count)

    edge = jnp.concatenate(
        [directions[:, 0, :].astype(jnp.float32).reshape(-1), magnitudes[:, :, 0].reshape(-1)]
    )
    edge = passed_back(edge, SLAB)
    packed = pack(outlier_rows, destinations, outlier_counts, slab_count, pair_cap)
    packed, edge = lax.optimization_barrier((packed, edge))
    arrived = lax.all_to_all(packed, SLAB, split_axis=0, concat_axis=0, tiled=True)

    edge_dirs = edge[: 2 * features].reshape(2, features)
    edge_mags = edge[2 * features :].reshape(4, heads, 1)
    factors = jnp.concatenate([magnitudes[:, :, 1:], edge_mags], axis=2)
    blocks = features // WIDTH
    factors = factors.reshape(4, blocks, heads // blocks, tokens).transpose(1, 3, 0, 2)
    factors = factors.reshape(blocks, tokens, 4 * heads // blocks)
    factors = jnp.pad(factors, ((0, 0), (0, 0), (0, 128 - factors.shape[2])))
    sequence = retention_order[0]
    positions = jnp.arange(tokens, dtype=jnp.int32)
    rank = jnp.sum(
        jnp.where(sequence[None, :] == positions[:, None], positions[None, :], 0), axis=1, keepdims=True
    )
    rank = jnp.broadcast_to(rank, (tokens, 128))
    factors, edge_dirs, rank = lax.optimization_barrier((factors, edge_dirs, rank))
    return place(arrived, rank, shift(directions, edge_dirs), factors)


def solution(mesh):
    finer = Mesh(
        mesh.devices.reshape(8, 4, 4, mesh.shape["head"]), ("slab_0", "slab_1", "slab_2", "head")
    )
    placed = (
        P(None, SLAB, "head"),
        P(None, "head", SLAB),
        P(SLAB, None, "head"),
        P(SLAB),
        P(SLAB, None),
        P(SLAB, None),
    )
    return jax.shard_map(
        per_device, mesh=finer, in_specs=placed, out_specs=P(None, SLAB, "head"), check_vma=False
    )
```

```python
import jax
import jax.numpy as jnp
from jax import lax
from jax.experimental import pallas as pl
from jax.experimental.pallas import tpu as pltpu
from jax.sharding import Mesh
from jax.sharding import PartitionSpec as P

SLAB = ("slab_0", "slab_1", "slab_2")
EMPTY = 2.0**127
WIDTH = 512
DEPTH = 2


def pack_kernel(pair_cap, dest_ref, count_ref, rows_ref, out_ref, held, blank, seen, slot, in_sem, out_sem):
    slabs = seen.shape[0]
    parts = in_sem.shape[0]
    size = held.shape[0] // parts

    def fetch(p):
        part = pl.ds(p * size, size)
        return pltpu.make_async_copy(rows_ref.at[part], held.at[part], in_sem.at[p])

    for p in range(parts):
        fetch(p).start()
    blank[...] = jnp.full(blank.shape, EMPTY, blank.dtype)

    def clear(i, carry):
        seen[i] = 0
        return carry

    lax.fori_loop(0, slabs, clear, 0, unroll=8)
    live = count_ref[0]

    def number(r, carry):
        d = dest_ref[r]
        j = seen[d]
        seen[d] = j + 1
        slot[r] = d * pair_cap + j
        return carry

    lax.fori_loop(0, live, number, 0)

    def leave(d, carry):
        for j in range(pair_cap):

            @pl.when(seen[d] <= j)
            def _():
                pltpu.make_async_copy(blank.at[0], out_ref.at[d * pair_cap + j], out_sem).start()

        return carry

    lax.fori_loop(0, slabs, leave, 0, unroll=4)
    for p in range(parts):
        fetch(p).wait()

    def send(r, carry):
        pltpu.make_async_copy(held.at[r], out_ref.at[slot[r]], out_sem).start()
        return carry

    lax.fori_loop(0, live, send, 0)
    pltpu.make_async_copy(out_ref, out_ref, out_sem).wait()


def pack(outlier_rows, destinations, outlier_counts, slab_count, pair_cap):
    row_slots, kinds, features = outlier_rows.shape
    smem = pl.BlockSpec(memory_space=pltpu.SMEM)
    anywhere = pl.BlockSpec(memory_space=pl.ANY)
    return pl.pallas_call(
        lambda *refs: pack_kernel(pair_cap, *refs),
        name="pack",
        in_specs=[smem, smem, anywhere],
        out_specs=anywhere,
        out_shape=jax.ShapeDtypeStruct((slab_count * pair_cap, kinds, features), outlier_rows.dtype),
        scratch_shapes=[
            pltpu.VMEM(outlier_rows.shape, outlier_rows.dtype),
            pltpu.VMEM((1, kinds, features), outlier_rows.dtype),
            pltpu.SMEM((slab_count,), jnp.int32),
            pltpu.SMEM((row_slots,), jnp.int32),
            pltpu.SemaphoreType.DMA((4,)),
            pltpu.SemaphoreType.DMA,
        ],
        cost_estimate=pl.CostEstimate(
            flops=0, bytes_accessed=3 * row_slots * kinds * features * 2, transcendentals=0
        ),
    )(destinations[:, 0], outlier_counts, outlier_rows)


def prepare_kernel(dirs_ref, order_ref, out_ref, rank_ref):
    tokens = dirs_ref.shape[1]
    for v in range(2):
        ahead = pltpu.roll(dirs_ref[v].astype(jnp.float32), tokens - 1, 0)
        out_ref[v] = ahead.astype(out_ref.dtype)

    @pl.when(pl.program_id(0) == 0)
    def _():
        token = lax.broadcasted_iota(jnp.int32, (tokens, tokens), 0)
        number = lax.broadcasted_iota(jnp.int32, (tokens, tokens), 1)
        here = jnp.where(order_ref[...] == token, number, 0).astype(jnp.float32)
        rank = jnp.sum(here, axis=1, keepdims=True).astype(jnp.int32)
        rank_ref[...] = jnp.broadcast_to(rank, rank_ref.shape)


def prepare(directions, order):
    _, tokens, features = directions.shape
    width = 256
    spec = pl.BlockSpec((2, tokens, width), lambda i: (0, 0, i))
    return pl.pallas_call(
        prepare_kernel,
        name="prepare",
        compiler_params=pltpu.CompilerParams(vmem_limit_bytes=16 * 2**20),
        grid=(features // width,),
        in_specs=[spec, pl.BlockSpec((1, tokens), lambda i: (0, 0))],
        out_specs=[spec, pl.BlockSpec((tokens, 128), lambda i: (0, 0))],
        out_shape=[
            jax.ShapeDtypeStruct(directions.shape, directions.dtype),
            jax.ShapeDtypeStruct((tokens, 128), jnp.int32),
        ],
        cost_estimate=pl.CostEstimate(
            flops=20 * tokens * features, bytes_accessed=8 * tokens * features, transcendentals=0
        ),
    )(directions, order)


def place_kernel(
    arrived, rank, dirs, mags, edge, out,
    a_buf, r_buf, d_buf, m_buf, e_buf, o_buf, placer, covered, wide,
    a_sem, r_sem, d_sem, m_sem, e_sem, o_sem,
):
    blocks, slots, kinds, width = a_buf.shape
    tokens = o_buf.shape[2]
    lanes = 128
    chunks = slots // lanes
    heads = width // lanes

    def columns(i):
        return pl.ds(pl.multiple_of(i * width, lanes), width)

    def a_copy(i):
        return pltpu.make_async_copy(arrived.at[:, :, columns(i)], a_buf.at[i], a_sem.at[i])

    def d_copy(i):
        return pltpu.make_async_copy(dirs.at[:, :, columns(i)], d_buf.at[i], d_sem.at[i])

    def o_copy(i):
        return pltpu.make_async_copy(o_buf.at[i], out.at[:, :, columns(i)], o_sem.at[i])

    r_copy = pltpu.make_async_copy(rank, r_buf, r_sem)
    m_copy = pltpu.make_async_copy(mags, m_buf, m_sem)
    e_copy = pltpu.make_async_copy(edge, e_buf, e_sem)
    a_copy(0).start()
    r_copy.start()
    m_copy.start()
    e_copy.start()
    d_copy(0).start()
    for i in range(1, DEPTH):
        a_copy(i).start()
        d_copy(i).start()

    r_copy.wait()
    m_copy.wait()
    e_copy.wait()

    def block(i, carry):
        @pl.when(i + DEPTH < blocks)
        def _():
            a_copy(i + DEPTH).start()
            d_copy(i + DEPTH).start()

        a_copy(i).wait()
        for c in range(heads):
            wide[c] = (
                a_buf[i, :, :, c * lanes : (c + 1) * lanes]
                .reshape(slots * kinds, lanes)
                .astype(jnp.float32)
            )

        @pl.when(i == 0)
        def _():
            first = wide[0, pl.ds(0, slots, stride=kinds), :]
            full = jnp.where(first < EMPTY, 1.0, 0.0).astype(jnp.bfloat16)
            corner = jnp.where(lax.broadcasted_iota(jnp.int32, (8, lanes), 1) == 0, 1.0, 0.0)
            corner = corner.astype(jnp.bfloat16)
            chunk = lax.broadcasted_iota(jnp.int32, (chunks, lanes), 0)
            over = (((1,), (1,)), ((), ()))
            filled = jnp.zeros((chunks, lanes), jnp.float32)
            for c in range(chunks):
                flags = lax.dot_general(
                    corner, full[c * lanes : (c + 1) * lanes], over, preferred_element_type=jnp.float32
                )
                filled = jnp.where(chunk == c, flags[0:1], filled)
            ones = filled.astype(jnp.bfloat16)
            source = lax.broadcasted_iota(jnp.int32, (lanes, lanes), 0)
            target = lax.broadcasted_iota(jnp.int32, (lanes, lanes), 1)
            tri = jnp.where(source < target, 1.0, 0.0).astype(jnp.bfloat16)
            inside = jnp.dot(ones, tri, preferred_element_type=jnp.float32)
            sums = jnp.dot(ones, jnp.ones((lanes, lanes), jnp.bfloat16), preferred_element_type=jnp.float32)
            ahead = jnp.zeros_like(sums)
            run = jnp.zeros((1, lanes), jnp.float32)
            for c in range(chunks):
                ahead = jnp.where(chunk == c, run, ahead)
                run = run + sums[c : c + 1]
            arrival = jnp.where(filled > 0.5, inside + ahead, -1.0).astype(jnp.int32)
            place_of = r_buf[...]
            covered[...] = jnp.where(place_of < run.astype(jnp.int32), 1, 0)
            for c in range(chunks):
                placer[:, c * lanes : (c + 1) * lanes] = jnp.where(
                    place_of == arrival[c : c + 1], 1.0, 0.0
                ).astype(jnp.bfloat16)

        d_copy(i).wait()
        tail = slice(tokens - 16, tokens)
        last = lax.broadcasted_iota(jnp.int32, (16, width), 0) == 15
        for v in range(2):
            end = d_buf[i, v, tail].astype(jnp.float32)
            end = jnp.where(last, e_buf[v : v + 1, columns(i)], end)
            d_buf[i, v, tail] = end.astype(d_buf.dtype)
        given = e_buf[2:3, pl.ds(pl.multiple_of(i * lanes, lanes), lanes)]
        m_buf[i, tail] = jnp.where(last[:, 0:lanes], given, m_buf[i, tail])
        factors = m_buf[i]
        own_dirs = [d_buf[i, v].astype(jnp.float32) for v in range(2)]
        taken = covered[...] > 0
        for k in range(kinds):
            rows = jnp.concatenate(
                [wide[c, pl.ds(k, slots, stride=kinds), :] for c in range(heads)], axis=1
            ).astype(jnp.bfloat16)
            inserted = jnp.dot(placer[...], rows, preferred_element_type=jnp.float32)
            for c in range(heads):
                part = slice(c * lanes, (c + 1) * lanes)
                own = factors[:, k * heads + c : k * heads + c + 1] * own_dirs[k % 2][:, part]
                o_buf[i, k, :, part] = jnp.where(taken, inserted[:, part], own).astype(o_buf.dtype)
        o_copy(i).start()
        return carry

    lax.fori_loop(0, blocks, block, 0)
    for i in range(blocks):
        o_copy(i).wait()


def place(arrived, rank, dirs, mags, edge):
    slots, kinds, features = arrived.shape
    _, tokens, _ = dirs.shape
    width = WIDTH
    blocks = features // width
    anywhere = pl.BlockSpec(memory_space=pl.ANY)
    return pl.pallas_call(
        place_kernel,
        name="place",
        in_specs=[anywhere] * 5,
        out_specs=anywhere,
        out_shape=jax.ShapeDtypeStruct((kinds, tokens, features), arrived.dtype),
        scratch_shapes=[
            pltpu.VMEM((blocks, slots, kinds, width), arrived.dtype),
            pltpu.VMEM(rank.shape, rank.dtype),
            pltpu.VMEM((blocks, 2, tokens, width), dirs.dtype),
            pltpu.VMEM(mags.shape, mags.dtype),
            pltpu.VMEM(edge.shape, edge.dtype),
            pltpu.VMEM((blocks, kinds, tokens, width), arrived.dtype),
            pltpu.VMEM((tokens, slots), jnp.bfloat16),
            pltpu.VMEM((tokens, 128), jnp.int32),
            pltpu.VMEM((width // 128, slots * kinds, 128), jnp.float32),
            pltpu.SemaphoreType.DMA((blocks,)),
            pltpu.SemaphoreType.DMA,
            pltpu.SemaphoreType.DMA((blocks,)),
            pltpu.SemaphoreType.DMA,
            pltpu.SemaphoreType.DMA,
            pltpu.SemaphoreType.DMA((blocks,)),
        ],
        cost_estimate=pl.CostEstimate(
            flops=2 * kinds * tokens * slots * features,
            bytes_accessed=2 * (slots * kinds + 2 * tokens + kinds * tokens) * features,
            transcendentals=0,
        ),
    )(arrived, rank, dirs, mags, edge)


def passed_back(block, axis):
    devices = lax.axis_size(axis)
    return lax.ppermute(block, axis, [((i + 1) % devices, i) for i in range(devices)])


def per_device(directions, magnitudes, outlier_rows, outlier_counts, destinations, retention_order):
    slab_count = lax.axis_size(SLAB)
    tokens, features = directions.shape[1], directions.shape[2]
    heads = magnitudes.shape[1]
    head_size = features // heads
    pair_cap = max(2, tokens // slab_count)

    packed = pack(outlier_rows, destinations, outlier_counts, slab_count, pair_cap)
    arrived = lax.all_to_all(packed, SLAB, split_axis=0, concat_axis=0, tiled=True)

    blocks = features // WIDTH

    def by_block(block):
        count = block.shape[2]
        block = block.reshape(4, blocks, heads // blocks, count).transpose(1, 3, 0, 2)
        block = block.reshape(blocks, count, 4 * heads // blocks)
        return jnp.pad(block, ((0, 0), (0, 0), (0, 128 - block.shape[2])))

    first_mags = by_block(magnitudes[:, :, :1]).reshape(1, blocks * 128)
    edge = jnp.concatenate(
        [
            directions[:, 0, :].astype(jnp.float32),
            jnp.pad(first_mags, ((0, 1), (0, features - blocks * 128))),
        ]
    )
    edge = passed_back(edge, SLAB)
    factors = by_block(jnp.roll(magnitudes, -1, axis=2))
    dirs, rank = prepare(directions, retention_order)
    return place(arrived, rank, dirs, factors, edge)


def solution(mesh):
    finer = Mesh(
        mesh.devices.reshape(8, 4, 4, mesh.shape["head"]), ("slab_0", "slab_1", "slab_2", "head")
    )
    placed = (
        P(None, SLAB, "head"),
        P(None, "head", SLAB),
        P(SLAB, None, "head"),
        P(SLAB),
        P(SLAB, None),
        P(SLAB, None),
    )
    return jax.shard_map(
        per_device, mesh=finer, in_specs=placed, out_specs=P(None, SLAB, "head"), check_vma=False
    )
```

```python
import jax
import jax.numpy as jnp
from jax import lax
from jax.experimental import pallas as pl
from jax.experimental.pallas import tpu as pltpu
from jax.sharding import Mesh
from jax.sharding import PartitionSpec as P

SLAB = ("slab_0", "slab_1", "slab_2")
EMPTY = 2.0**127
WIDTH = 512
DEPTH = 2


def pack_kernel(pair_cap, dest_ref, count_ref, rows_ref, out_ref, held, blank, seen, slot, in_sem, out_sem):
    slabs = seen.shape[0]
    parts = in_sem.shape[0]
    kinds = held.shape[1]
    size = held.shape[0] // parts

    def fetch(p):
        part = pl.ds(p * size, size)
        return pltpu.make_async_copy(rows_ref.at[part], held.at[part], in_sem.at[p])

    for p in range(parts):
        fetch(p).start()
    blank[...] = jnp.full(blank.shape, EMPTY, blank.dtype)

    def clear(i, carry):
        seen[i] = 0
        return carry

    lax.fori_loop(0, slabs, clear, 0, unroll=8)
    live = count_ref[0]

    def number(r, carry):
        d = dest_ref[r]
        j = seen[d]
        seen[d] = j + 1
        slot[r] = j
        return carry

    lax.fori_loop(0, live, number, 0)

    def leave(d, carry):
        for j in range(pair_cap):

            @pl.when(seen[d] <= j)
            def _():
                pltpu.make_async_copy(
                    blank.at[0], out_ref.at[d, pl.ds(j * kinds, kinds)], out_sem
                ).start()

        return carry

    lax.fori_loop(0, slabs, leave, 0, unroll=4)
    for p in range(parts):
        fetch(p).wait()

    def send(r, carry):
        d = dest_ref[r]
        first = pl.multiple_of(slot[r] * kinds, kinds)
        pltpu.make_async_copy(held.at[r], out_ref.at[d, pl.ds(first, kinds)], out_sem).start()
        return carry

    lax.fori_loop(0, live, send, 0)
    pltpu.make_async_copy(out_ref, out_ref, out_sem).wait()


def pack(outlier_rows, destinations, outlier_counts, slab_count, pair_cap):
    row_slots, kinds, features = outlier_rows.shape
    smem = pl.BlockSpec(memory_space=pltpu.SMEM)
    anywhere = pl.BlockSpec(memory_space=pl.ANY)
    return pl.pallas_call(
        lambda *refs: pack_kernel(pair_cap, *refs),
        name="pack",
        in_specs=[smem, smem, anywhere],
        out_specs=anywhere,
        out_shape=jax.ShapeDtypeStruct((slab_count, pair_cap * kinds, features), outlier_rows.dtype),
        scratch_shapes=[
            pltpu.VMEM(outlier_rows.shape, outlier_rows.dtype),
            pltpu.VMEM((1, kinds, features), outlier_rows.dtype),
            pltpu.SMEM((slab_count,), jnp.int32),
            pltpu.SMEM((row_slots,), jnp.int32),
            pltpu.SemaphoreType.DMA((4,)),
            pltpu.SemaphoreType.DMA,
        ],
        cost_estimate=pl.CostEstimate(
            flops=0, bytes_accessed=3 * row_slots * kinds * features * 2, transcendentals=0
        ),
    )(destinations[:, 0], outlier_counts, outlier_rows)


def prepare_kernel(dirs_ref, order_ref, out_ref, rank_ref):
    tokens = dirs_ref.shape[1]
    for v in range(2):
        ahead = pltpu.roll(dirs_ref[v].astype(jnp.float32), tokens - 1, 0)
        out_ref[v] = ahead.astype(out_ref.dtype)

    @pl.when(pl.program_id(0) == 0)
    def _():
        token = lax.broadcasted_iota(jnp.int32, (tokens, tokens), 0)
        number = lax.broadcasted_iota(jnp.int32, (tokens, tokens), 1)
        here = jnp.where(order_ref[...] == token, number, 0).astype(jnp.float32)
        rank = jnp.sum(here, axis=1, keepdims=True).astype(jnp.int32)
        rank_ref[...] = jnp.broadcast_to(rank, rank_ref.shape)


def prepare(directions, order):
    _, tokens, features = directions.shape
    width = 256
    spec = pl.BlockSpec((2, tokens, width), lambda i: (0, 0, i))
    return pl.pallas_call(
        prepare_kernel,
        name="prepare",
        compiler_params=pltpu.CompilerParams(vmem_limit_bytes=16 * 2**20),
        grid=(features // width,),
        in_specs=[spec, pl.BlockSpec((1, tokens), lambda i: (0, 0))],
        out_specs=[spec, pl.BlockSpec((tokens, 128), lambda i: (0, 0))],
        out_shape=[
            jax.ShapeDtypeStruct(directions.shape, directions.dtype),
            jax.ShapeDtypeStruct((tokens, 128), jnp.int32),
        ],
        cost_estimate=pl.CostEstimate(
            flops=20 * tokens * features, bytes_accessed=8 * tokens * features, transcendentals=0
        ),
    )(directions, order)


def place_kernel(
    arrived, rank, dirs, mags, edge, out,
    a_buf, r_buf, d_buf, m_buf, e_buf, o_buf, placer, covered, wide,
    a_sem, r_sem, d_sem, m_sem, e_sem, o_sem,
):
    blocks, kinds, tokens, width = o_buf.shape
    slots = a_buf.shape[1] * a_buf.shape[2] // kinds
    lanes = 128
    chunks = slots // lanes
    heads = width // lanes

    def columns(i):
        return pl.ds(pl.multiple_of(i * width, lanes), width)

    def a_copy(i):
        return pltpu.make_async_copy(arrived.at[:, :, columns(i)], a_buf.at[i], a_sem.at[i])

    def d_copy(i):
        return pltpu.make_async_copy(dirs.at[:, :, columns(i)], d_buf.at[i], d_sem.at[i])

    def o_copy(i):
        return pltpu.make_async_copy(o_buf.at[i], out.at[:, :, columns(i)], o_sem.at[i])

    r_copy = pltpu.make_async_copy(rank, r_buf, r_sem)
    m_copy = pltpu.make_async_copy(mags, m_buf, m_sem)
    e_copy = pltpu.make_async_copy(edge, e_buf, e_sem)
    a_copy(0).start()
    r_copy.start()
    m_copy.start()
    e_copy.start()
    d_copy(0).start()
    for i in range(1, DEPTH):
        a_copy(i).start()
        d_copy(i).start()


    def block(i, carry):
        @pl.when(i + DEPTH < blocks)
        def _():
            a_copy(i + DEPTH).start()
            d_copy(i + DEPTH).start()

        a_copy(i).wait()
        for c in range(heads):
            wide[c] = (
                a_buf[i, :, :, c * lanes : (c + 1) * lanes]
                .reshape(slots * kinds, lanes)
                .astype(jnp.float32)
            )

        @pl.when(i == 0)
        def _():
            first = wide[0, pl.ds(0, slots, stride=kinds), :]
            full = jnp.where(first < EMPTY, 1.0, 0.0).astype(jnp.bfloat16)
            corner = jnp.where(lax.broadcasted_iota(jnp.int32, (8, lanes), 1) == 0, 1.0, 0.0)
            corner = corner.astype(jnp.bfloat16)
            chunk = lax.broadcasted_iota(jnp.int32, (chunks, lanes), 0)
            over = (((1,), (1,)), ((), ()))
            filled = jnp.zeros((chunks, lanes), jnp.float32)
            for c in range(chunks):
                flags = lax.dot_general(
                    corner, full[c * lanes : (c + 1) * lanes], over, preferred_element_type=jnp.float32
                )
                filled = jnp.where(chunk == c, flags[0:1], filled)
            ones = filled.astype(jnp.bfloat16)
            source = lax.broadcasted_iota(jnp.int32, (lanes, lanes), 0)
            target = lax.broadcasted_iota(jnp.int32, (lanes, lanes), 1)
            tri = jnp.where(source < target, 1.0, 0.0).astype(jnp.bfloat16)
            inside = jnp.dot(ones, tri, preferred_element_type=jnp.float32)
            sums = jnp.dot(ones, jnp.ones((lanes, lanes), jnp.bfloat16), preferred_element_type=jnp.float32)
            ahead = jnp.zeros_like(sums)
            run = jnp.zeros((1, lanes), jnp.float32)
            for c in range(chunks):
                ahead = jnp.where(chunk == c, run, ahead)
                run = run + sums[c : c + 1]
            arrival = jnp.where(filled > 0.5, inside + ahead, -1.0).astype(jnp.int32)
            r_copy.wait()
            m_copy.wait()
            e_copy.wait()
            place_of = r_buf[...]
            covered[...] = jnp.where(place_of < run.astype(jnp.int32), 1, 0)
            for c in range(chunks):
                placer[:, c * lanes : (c + 1) * lanes] = jnp.where(
                    place_of == arrival[c : c + 1], 1.0, 0.0
                ).astype(jnp.bfloat16)

        d_copy(i).wait()
        tail = slice(tokens - 16, tokens)
        last = lax.broadcasted_iota(jnp.int32, (16, width), 0) == 15
        for v in range(2):
            end = d_buf[i, v, tail].astype(jnp.float32)
            end = jnp.where(last, e_buf[v : v + 1, columns(i)], end)
            d_buf[i, v, tail] = end.astype(d_buf.dtype)
        given = e_buf[2:3, pl.ds(pl.multiple_of(i * lanes, lanes), lanes)]
        m_buf[i, tail] = jnp.where(last[:, 0:lanes], given, m_buf[i, tail])
        factors = jnp.where(covered[...] > 0, 0.0, m_buf[i])
        own_dirs = [d_buf[i, v].astype(jnp.float32) for v in range(2)]
        for k in range(kinds):
          for c0 in range(0, heads, 2):
            rows = jnp.concatenate(
                [wide[c, pl.ds(k, slots, stride=kinds), :] for c in range(c0, c0 + 2)], axis=1
            ).astype(jnp.bfloat16)
            both = jnp.dot(placer[...], rows, preferred_element_type=jnp.float32)
            for c in range(c0, c0 + 2):
                part = slice(c * lanes, (c + 1) * lanes)
                got = both[:, (c - c0) * lanes : (c - c0 + 1) * lanes]
                own = factors[:, k * heads + c : k * heads + c + 1] * own_dirs[k % 2][:, part]
                o_buf[i, k, :, part] = (got + own).astype(o_buf.dtype)
        o_copy(i).start()
        return carry

    lax.fori_loop(0, blocks, block, 0)
    for i in range(blocks):
        o_copy(i).wait()


def place(arrived, rank, dirs, mags, edge):
    slabs, group, features = arrived.shape
    kinds = 4
    slots = slabs * group // kinds
    _, tokens, _ = dirs.shape
    width = WIDTH
    blocks = features // width
    anywhere = pl.BlockSpec(memory_space=pl.ANY)
    return pl.pallas_call(
        place_kernel,
        name="place",
        in_specs=[anywhere] * 5,
        out_specs=anywhere,
        out_shape=jax.ShapeDtypeStruct((kinds, tokens, features), arrived.dtype),
        scratch_shapes=[
            pltpu.VMEM((blocks, slabs, group, width), arrived.dtype),
            pltpu.VMEM(rank.shape, rank.dtype),
            pltpu.VMEM((blocks, 2, tokens, width), dirs.dtype),
            pltpu.VMEM(mags.shape, mags.dtype),
            pltpu.VMEM(edge.shape, edge.dtype),
            pltpu.VMEM((blocks, kinds, tokens, width), arrived.dtype),
            pltpu.VMEM((tokens, slots), jnp.bfloat16),
            pltpu.VMEM((tokens, 128), jnp.int32),
            pltpu.VMEM((width // 128, slots * kinds, 128), jnp.float32),
            pltpu.SemaphoreType.DMA((blocks,)),
            pltpu.SemaphoreType.DMA,
            pltpu.SemaphoreType.DMA((blocks,)),
            pltpu.SemaphoreType.DMA,
            pltpu.SemaphoreType.DMA,
            pltpu.SemaphoreType.DMA((blocks,)),
        ],
        cost_estimate=pl.CostEstimate(
            flops=2 * kinds * tokens * slots * features,
            bytes_accessed=2 * (slots * kinds + 2 * tokens + kinds * tokens) * features,
            transcendentals=0,
        ),
    )(arrived, rank, dirs, mags, edge)


def passed_back(block, axis):
    devices = lax.axis_size(axis)
    return lax.ppermute(block, axis, [((i + 1) % devices, i) for i in range(devices)])


def per_device(directions, magnitudes, outlier_rows, outlier_counts, destinations, retention_order):
    slab_count = lax.axis_size(SLAB)
    tokens, features = directions.shape[1], directions.shape[2]
    heads = magnitudes.shape[1]
    head_size = features // heads
    pair_cap = max(2, tokens // slab_count)

    packed = pack(outlier_rows, destinations, outlier_counts, slab_count, pair_cap)
    arrived = lax.all_to_all(packed, SLAB, split_axis=0, concat_axis=0, tiled=True)

    blocks = features // WIDTH

    def by_block(block):
        count = block.shape[2]
        block = block.reshape(4, blocks, heads // blocks, count).transpose(1, 3, 0, 2)
        block = block.reshape(blocks, count, 4 * heads // blocks)
        return jnp.pad(block, ((0, 0), (0, 0), (0, 128 - block.shape[2])))

    first_mags = by_block(magnitudes[:, :, :1]).reshape(1, blocks * 128)
    edge = jnp.concatenate(
        [
            directions[:, 0, :].astype(jnp.float32),
            jnp.pad(first_mags, ((0, 1), (0, features - blocks * 128))),
        ]
    )
    edge = passed_back(edge, SLAB)
    factors = by_block(jnp.roll(magnitudes, -1, axis=2))
    dirs, rank = prepare(directions, retention_order)
    return place(arrived, rank, dirs, factors, edge)


def solution(mesh):
    finer = Mesh(
        mesh.devices.reshape(8, 4, 4, mesh.shape["head"]), ("slab_0", "slab_1", "slab_2", "head")
    )
    placed = (
        P(None, SLAB, "head"),
        P(None, "head", SLAB),
        P(SLAB, None, "head"),
        P(SLAB),
        P(SLAB, None),
        P(SLAB, None),
    )
    return jax.shard_map(
        per_device, mesh=finer, in_specs=placed, out_specs=P(None, SLAB, "head"), check_vma=False
    )
```

```python
import jax
import jax.numpy as jnp
from jax import lax
from jax.experimental import pallas as pl
from jax.experimental.pallas import tpu as pltpu
from jax.sharding import Mesh
from jax.sharding import PartitionSpec as P


SLAB = ("slab_0", "slab_1", "slab_2")
EMPTY = 2.0**127
WIDTH = 512
DEPTH = 2
SPILL = 5


def pack_kernel(turn, dest_ref, count_ref, rows_ref, out_ref, held, blank, seen, slot, in_sem, out_sem):
    slabs = out_ref.shape[0]
    parts = in_sem.shape[0]
    size = held.shape[0] // parts

    def fetch(p):
        part = pl.ds(p * size, size)
        return pltpu.make_async_copy(rows_ref.at[part], held.at[part], in_sem.at[p])

    for p in range(parts):
        fetch(p).start()
    blank[...] = jnp.full(blank.shape, EMPTY, blank.dtype)

    def clear(i, carry):
        seen[i] = 0
        return carry

    lax.fori_loop(0, slabs, clear, 0, unroll=8)
    live = count_ref[0]

    def number(r, carry):
        d = dest_ref[r]
        j = seen[d]
        seen[d] = j + 1
        slot[r] = jnp.where(j == turn, d, -1)
        return carry

    lax.fori_loop(0, live, number, 0)

    def leave(d, carry):
        @pl.when(seen[d] <= turn)
        def _():
            pltpu.make_async_copy(blank.at[0], out_ref.at[d], out_sem).start()

        return carry

    lax.fori_loop(0, slabs, leave, 0, unroll=4)
    for p in range(parts):
        fetch(p).wait()

    def send(r, carry):
        @pl.when(slot[r] >= 0)
        def _():
            pltpu.make_async_copy(held.at[r], out_ref.at[slot[r]], out_sem).start()

        return carry

    lax.fori_loop(0, live, send, 0)
    pltpu.make_async_copy(out_ref, out_ref, out_sem).wait()


def pack(outlier_rows, destinations, outlier_counts, slab_count, turn):
    row_slots, kinds, features = outlier_rows.shape
    smem = pl.BlockSpec(memory_space=pltpu.SMEM)
    anywhere = pl.BlockSpec(memory_space=pl.ANY)
    return pl.pallas_call(
        lambda *refs: pack_kernel(turn, *refs),
        name="pack",
        in_specs=[smem, smem, anywhere],
        out_specs=anywhere,
        out_shape=jax.ShapeDtypeStruct((slab_count, kinds, features), outlier_rows.dtype),
        scratch_shapes=[
            pltpu.VMEM(outlier_rows.shape, outlier_rows.dtype),
            pltpu.VMEM((1, kinds, features), outlier_rows.dtype),
            pltpu.SMEM((slab_count,), jnp.int32),
            pltpu.SMEM((row_slots,), jnp.int32),
            pltpu.SemaphoreType.DMA((4,)),
            pltpu.SemaphoreType.DMA,
        ],
        cost_estimate=pl.CostEstimate(
            flops=2000000, bytes_accessed=2 * row_slots * kinds * features * 2, transcendentals=0
        ),
    )(destinations[:, 0], outlier_counts, outlier_rows)


def spill_kernel(plane, dest_ref, count_ref, rows_ref, out_ref, seen, filled, mark, sem):
    slabs = seen.shape[0]
    planes = filled.shape[0]
    places = out_ref.shape[0]
    cap = places // planes
    kinds = out_ref.shape[1]
    features = rows_ref.shape[2]

    def blank(i, carry):
        out_ref[i] = jnp.full(out_ref.shape[1:], EMPTY, out_ref.dtype)
        mark[i] = plane
        return carry

    lax.fori_loop(0, places, blank, 0)

    def clear(i, carry):
        seen[i] = 0
        return carry

    lax.fori_loop(0, slabs, clear, 0, unroll=8)
    for p in range(planes):
        filled[p] = 0
    live = count_ref[0]

    def send(r, started):
        d = dest_ref[r]
        j = seen[d]
        seen[d] = j + 1
        p = lax.div(d, plane)
        e = filled[p]
        fits = (j > 0) & (e < cap)
        filled[p] = e + jnp.where(j > 0, 1, 0)

        @pl.when(fits)
        def _():
            at = p * cap + e
            mark[at] = d - p * plane
            pltpu.make_async_copy(
                rows_ref.at[r], out_ref.at[at, :, pl.ds(0, features)], sem
            ).start()

        return started + jnp.where(fits, 1, 0)

    started = lax.fori_loop(0, live, send, 0)
    most = filled[0]
    for p in range(1, planes):
        most = jnp.maximum(most, filled[p])
    over = jnp.where(most > cap, 2 * plane, 0)

    def label(i, carry):
        value = (mark[i] + over).astype(jnp.float32)
        out_ref[i, :, pl.ds(features, 128)] = jnp.full((kinds, 128), value).astype(out_ref.dtype)
        return carry

    lax.fori_loop(0, places, label, 0)

    def finish(r, carry):
        pltpu.make_async_copy(rows_ref.at[0], out_ref.at[0, :, pl.ds(0, features)], sem).wait()
        return carry

    lax.fori_loop(0, started, finish, 0)


def spill(outlier_rows, destinations, outlier_counts, slab_count, planes):
    _, kinds, features = outlier_rows.shape
    smem = pl.BlockSpec(memory_space=pltpu.SMEM)
    plane = slab_count // planes
    return pl.pallas_call(
        lambda *refs: spill_kernel(plane, *refs),
        name="spill",
        in_specs=[smem, smem, pl.BlockSpec(memory_space=pl.ANY)],
        out_specs=pl.BlockSpec(memory_space=pltpu.VMEM),
        out_shape=jax.ShapeDtypeStruct((planes * SPILL, kinds, features + 128), outlier_rows.dtype),
        scratch_shapes=[
            pltpu.SMEM((slab_count,), jnp.int32),
            pltpu.SMEM((planes,), jnp.int32),
            pltpu.SMEM((planes * SPILL,), jnp.int32),
            pltpu.SemaphoreType.DMA,
        ],
        cost_estimate=pl.CostEstimate(
            flops=2000000, bytes_accessed=4 * planes * SPILL * kinds * features, transcendentals=0
        ),
    )(destinations[:, 0], outlier_counts, outlier_rows)


def relay_kernel(here_ref, in_ref, *out_refs):
    places, kinds, width = in_ref.shape
    count = len(out_refs)
    senders = out_refs[0].shape[0]
    cap = places // senders
    total = places * kinds
    lanes = 128
    rows = in_ref[...].reshape(total, width)
    labels = rows[:, width - lanes :]
    corner = jnp.where(lax.broadcasted_iota(jnp.int32, (8, lanes), 1) == 0, 1.0, 0.0).astype(jnp.bfloat16)
    over = (((1,), (1,)), ((), ()))
    label = lax.dot_general(corner, labels, over, preferred_element_type=jnp.float32)[0:1]
    label = label.astype(jnp.int32)
    full = jnp.max(label, axis=1, keepdims=True) >= 2 * count
    owner = label & (2 * count - 1)
    x, y = here_ref[0], here_ref[1]
    ahead = (((owner >> 2) - x) & 3) * 4 + (((owner & 3) - y) & 3)
    ahead = jnp.where(owner < count, ahead, count)
    source = lax.broadcasted_iota(jnp.int32, (senders * kinds, total), 1)
    target = lax.broadcasted_iota(jnp.int32, (senders * kinds, total), 0)
    same = (source % kinds == target % kinds) & (source // (cap * kinds) == target // kinds)
    told = jnp.where(full, 1.0, 0.0) * jnp.ones((senders * kinds, lanes), jnp.float32)
    for o in range(count):
        picker = jnp.where(same & (ahead == o), 1.0, 0.0)
        any_ = jnp.sum(picker, axis=1, keepdims=True) > 0.5
        got = jnp.dot(picker.astype(jnp.bfloat16), rows, preferred_element_type=jnp.float32)
        got = jnp.where(any_, got, EMPTY)
        got = jnp.concatenate([got[:, : width - lanes], told], axis=1)
        out_refs[o][...] = got.reshape(senders, kinds, width).astype(out_refs[o].dtype)


def relay(gathered, here, planes, count):
    _, kinds, width = gathered.shape
    return pl.pallas_call(
        relay_kernel,
        name="relay",
        in_specs=[pl.BlockSpec(memory_space=pltpu.SMEM), pl.BlockSpec(memory_space=pltpu.VMEM)],
        out_specs=[pl.BlockSpec(memory_space=pltpu.VMEM)] * count,
        out_shape=[jax.ShapeDtypeStruct((planes, kinds, width), gathered.dtype)] * count,
        cost_estimate=pl.CostEstimate(
            flops=10000000, bytes_accessed=4 * count * planes * kinds * width, transcendentals=0
        ),
    )(here, gathered)


def prepare_kernel(dirs_ref, order_ref, out_ref, rank_ref):
    tokens = dirs_ref.shape[1]
    for v in range(2):
        ahead = pltpu.roll(dirs_ref[v].astype(jnp.float32), tokens - 1, 0)
        out_ref[v] = ahead.astype(out_ref.dtype)

    @pl.when(pl.program_id(0) == 0)
    def _():
        token = lax.broadcasted_iota(jnp.int32, (tokens, tokens), 0)
        number = lax.broadcasted_iota(jnp.int32, (tokens, tokens), 1)
        here = jnp.where(order_ref[...] == token, number, 0).astype(jnp.float32)
        rank = jnp.sum(here, axis=1, keepdims=True).astype(jnp.int32)
        rank_ref[...] = jnp.broadcast_to(rank, rank_ref.shape)


def prepare(directions, order):
    _, tokens, features = directions.shape
    width = 256
    spec = pl.BlockSpec((2, tokens, width), lambda i: (0, 0, i))
    return pl.pallas_call(
        prepare_kernel,
        name="prepare",
        compiler_params=pltpu.CompilerParams(vmem_limit_bytes=16 * 2**20),
        grid=(features // width,),
        in_specs=[spec, pl.BlockSpec((1, tokens), lambda i: (0, 0))],
        out_specs=[spec, pl.BlockSpec((tokens, 128), lambda i: (0, 0))],
        out_shape=[
            jax.ShapeDtypeStruct(directions.shape, directions.dtype),
            jax.ShapeDtypeStruct((tokens, 128), jnp.int32),
        ],
        cost_estimate=pl.CostEstimate(
            flops=20 * tokens * features, bytes_accessed=8 * tokens * features, transcendentals=0
        ),
    )(directions, order)


def place_kernel(
    first, second, order, rank, dirs, mags, edge, out,
    a_buf, k_buf, r_buf, d_buf, m_buf, e_buf, o_buf, placer, covered, wide,
    a_sem, k_sem, r_sem, d_sem, m_sem, e_sem, o_sem,
):
    blocks, kinds, tokens, width = o_buf.shape
    slots = a_buf.shape[1]
    half = slots // 2
    lanes = 128
    chunks = slots // lanes
    heads = width // lanes

    def columns(i):
        return pl.ds(pl.multiple_of(i * width, lanes), width)

    class a_copy:
        def __init__(self, i):
            self.parts = [
                pltpu.make_async_copy(
                    half_of.at[:, :, columns(i)], a_buf.at[i, pl.ds(j * half, half)], a_sem.at[i, j]
                )
                for j, half_of in enumerate((first, second))
            ]

        def start(self):
            for part in self.parts:
                part.start()

        def wait(self):
            for part in self.parts:
                part.wait()

    def d_copy(i):
        return pltpu.make_async_copy(dirs.at[:, :, columns(i)], d_buf.at[i], d_sem.at[i])

    def o_copy(i):
        return pltpu.make_async_copy(o_buf.at[i], out.at[:, :, columns(i)], o_sem.at[i])

    r_copy = pltpu.make_async_copy(rank, r_buf, r_sem)
    k_copy = pltpu.make_async_copy(order, k_buf, k_sem)
    m_copy = pltpu.make_async_copy(mags, m_buf, m_sem)
    e_copy = pltpu.make_async_copy(edge, e_buf, e_sem)
    a_copy(0).start()
    k_copy.start()
    r_copy.start()
    m_copy.start()
    e_copy.start()
    d_copy(0).start()
    for i in range(1, DEPTH):
        a_copy(i).start()
        d_copy(i).start()


    def block(i, carry):
        @pl.when(i + DEPTH < blocks)
        def _():
            a_copy(i + DEPTH).start()
            d_copy(i + DEPTH).start()

        a_copy(i).wait()
        for c in range(heads):
            wide[c] = (
                a_buf[i, :, :, c * lanes : (c + 1) * lanes]
                .reshape(slots * kinds, lanes)
                .astype(jnp.float32)
            )

        @pl.when(i == 0)
        def _():
            corner_of = wide[0, pl.ds(0, slots, stride=kinds), :]
            full = jnp.where(corner_of < EMPTY, 1.0, 0.0).astype(jnp.bfloat16)
            corner = jnp.where(lax.broadcasted_iota(jnp.int32, (8, lanes), 1) == 0, 1.0, 0.0)
            corner = corner.astype(jnp.bfloat16)
            over = (((1,), (1,)), ((), ()))
            filled = [
                lax.dot_general(
                    corner, full[c * lanes : (c + 1) * lanes], over, preferred_element_type=jnp.float32
                )
                for c in range(chunks)
            ]
            run = jnp.sum(sum(filled), axis=1, keepdims=True)[0:1]
            k_copy.wait()
            ahead = []
            for c in range(chunks):
                number = jnp.zeros((8, lanes), jnp.float32)
                for e in range(chunks):
                    earlier = k_buf[e, :, :] < k_buf[2 + c, 0:1, :]
                    number += jnp.dot(
                        filled[e].astype(jnp.bfloat16),
                        jnp.where(earlier, 1.0, 0.0).astype(jnp.bfloat16),
                        preferred_element_type=jnp.float32,
                    )
                ahead.append(jnp.where(filled[c] > 0.5, number, -1.0).astype(jnp.int32))
            r_copy.wait()
            m_copy.wait()
            e_copy.wait()
            place_of = r_buf[...]
            covered[...] = jnp.where(place_of < run.astype(jnp.int32), 1, 0)
            for c in range(chunks):
                placer[:, c * lanes : (c + 1) * lanes] = jnp.where(
                    place_of == ahead[c][0:1], 1.0, 0.0
                ).astype(jnp.bfloat16)

        d_copy(i).wait()
        tail = slice(tokens - 16, tokens)
        last = lax.broadcasted_iota(jnp.int32, (16, width), 0) == 15
        for v in range(2):
            end = d_buf[i, v, tail].astype(jnp.float32)
            end = jnp.where(last, e_buf[v : v + 1, columns(i)], end)
            d_buf[i, v, tail] = end.astype(d_buf.dtype)
        given = e_buf[2:3, pl.ds(pl.multiple_of(i * lanes, lanes), lanes)]
        m_buf[i, tail] = jnp.where(last[:, 0:lanes], given, m_buf[i, tail])
        factors = jnp.where(covered[...] > 0, 0.0, m_buf[i])
        own_dirs = [d_buf[i, v].astype(jnp.float32) for v in range(2)]
        for k in range(kinds):
          for c0 in range(0, heads, 2):
            rows = jnp.concatenate(
                [wide[c, pl.ds(k, slots, stride=kinds), :] for c in range(c0, c0 + 2)], axis=1
            ).astype(jnp.bfloat16)
            both = jnp.dot(placer[...], rows, preferred_element_type=jnp.float32)
            for c in range(c0, c0 + 2):
                part = slice(c * lanes, (c + 1) * lanes)
                got = both[:, (c - c0) * lanes : (c - c0 + 1) * lanes]
                own = factors[:, k * heads + c : k * heads + c + 1] * own_dirs[k % 2][:, part]
                o_buf[i, k, :, part] = (got + own).astype(o_buf.dtype)
        o_copy(i).start()
        return carry

    lax.fori_loop(0, blocks, block, 0)
    for i in range(blocks):
        o_copy(i).wait()


def place(first, second, order, rank, dirs, mags, edge):
    slabs, kinds, features = first.shape
    slots = 2 * slabs
    _, tokens, _ = dirs.shape
    width = WIDTH
    blocks = features // width
    anywhere = pl.BlockSpec(memory_space=pl.ANY)
    return pl.pallas_call(
        place_kernel,
        name="place",
        in_specs=[anywhere] * 7,
        out_specs=anywhere,
        out_shape=jax.ShapeDtypeStruct((kinds, tokens, features), first.dtype),
        scratch_shapes=[
            pltpu.VMEM((blocks, slots, kinds, width), first.dtype),
            pltpu.VMEM(order.shape, order.dtype),
            pltpu.VMEM(rank.shape, rank.dtype),
            pltpu.VMEM((blocks, 2, tokens, width), dirs.dtype),
            pltpu.VMEM(mags.shape, mags.dtype),
            pltpu.VMEM(edge.shape, edge.dtype),
            pltpu.VMEM((blocks, kinds, tokens, width), first.dtype),
            pltpu.VMEM((tokens, slots), jnp.bfloat16),
            pltpu.VMEM((tokens, 128), jnp.int32),
            pltpu.VMEM((width // 128, slots * kinds, 128), jnp.float32),
            pltpu.SemaphoreType.DMA((blocks, 2)),
            pltpu.SemaphoreType.DMA,
            pltpu.SemaphoreType.DMA,
            pltpu.SemaphoreType.DMA((blocks,)),
            pltpu.SemaphoreType.DMA,
            pltpu.SemaphoreType.DMA,
            pltpu.SemaphoreType.DMA((blocks,)),
        ],
        cost_estimate=pl.CostEstimate(
            flops=2 * kinds * tokens * slots * features,
            bytes_accessed=2 * (slots * kinds + 2 * tokens + kinds * tokens) * features,
            transcendentals=0,
        ),
    )(first, second, order, rank, dirs, mags, edge)


def passed_back(block, axis):
    devices = lax.axis_size(axis)
    return lax.ppermute(block, axis, [((i + 1) % devices, i) for i in range(devices)])


def per_device(directions, magnitudes, outlier_rows, outlier_counts, destinations, retention_order):
    slab_count = lax.axis_size(SLAB)
    tokens, features = directions.shape[1], directions.shape[2]
    heads = magnitudes.shape[1]
    head_size = features // heads
    planes = lax.axis_size("slab_0")
    plane = ("slab_1", "slab_2")
    wide, deep = lax.axis_size("slab_1"), lax.axis_size("slab_2")
    x, y = lax.axis_index("slab_1"), lax.axis_index("slab_2")

    spilled = spill(outlier_rows, destinations, outlier_counts, slab_count, planes)
    gathered = lax.all_to_all(spilled, "slab_0", split_axis=0, concat_axis=0, tiled=True)
    packed = pack(outlier_rows, destinations, outlier_counts, slab_count, 0)
    packed, gathered = lax.optimization_barrier((packed, gathered))
    first = lax.all_to_all(packed, SLAB, split_axis=0, concat_axis=0, tiled=True)

    sorted_rows = relay(gathered, jnp.stack([x, y]).astype(jnp.int32), planes, wide * deep)
    steps = [(dx, dy) for dx in range(wide) for dy in range(deep)]
    second = []
    for (dx, dy), rows in zip(steps, sorted_rows):
        if (dx, dy) != (0, 0):
            route = [
                (i * deep + j, (i + dx) % wide * deep + (j + dy) % deep)
                for i in range(wide)
                for j in range(deep)
            ]
            rows = lax.ppermute(rows, plane, route)
        second.append(rows)
    second = jnp.concatenate(second, axis=0)
    too_many = jnp.max(second[:, 0, features]) > 0.5

    slabs = jnp.arange(slab_count, dtype=jnp.int32)
    step, z = slabs // planes, slabs % planes
    came = z * (wide * deep) + (x - step // deep) % wide * deep + (y - step % deep) % deep

    def order_of(first_slab, second_slab):
        keys = jnp.stack([2 * first_slab, 2 * second_slab + 1]).astype(jnp.int32)
        return jnp.concatenate(
            [
                jnp.broadcast_to(keys[:, :, None], (2, slab_count, 128)),
                jnp.broadcast_to(keys[:, None, :], (2, slab_count, 128)),
            ]
        )

    blocks = features // WIDTH

    def by_block(block):
        count = block.shape[2]
        block = block.reshape(4, blocks, heads // blocks, count).transpose(1, 3, 0, 2)
        block = block.reshape(blocks, count, 4 * heads // blocks)
        return jnp.pad(block, ((0, 0), (0, 0), (0, 128 - block.shape[2])))

    first_mags = by_block(magnitudes[:, :, :1]).reshape(1, blocks * 128)
    edge = jnp.concatenate(
        [
            directions[:, 0, :].astype(jnp.float32),
            jnp.pad(first_mags, ((0, 1), (0, features - blocks * 128))),
        ]
    )
    edge = passed_back(edge, SLAB)
    factors = by_block(jnp.roll(magnitudes, -1, axis=2))
    dirs, rank = prepare(directions, retention_order)
    relayed, direct = order_of(slabs, came), order_of(slabs, slabs)

    def short(_):
        return place(first, second, relayed, rank, dirs, factors, edge)

    def long(_):
        rest = pack(outlier_rows, destinations, outlier_counts, slab_count, 1)
        rest = lax.all_to_all(rest, SLAB, split_axis=0, concat_axis=0, tiled=True)
        return place(first, rest, direct, rank, dirs, factors, edge)

    return lax.cond(too_many, long, short, 0)


def solution(mesh):
    finer = Mesh(
        mesh.devices.reshape(8, 4, 4, mesh.shape["head"]), ("slab_0", "slab_1", "slab_2", "head")
    )
    placed = (
        P(None, SLAB, "head"),
        P(None, "head", SLAB),
        P(SLAB, None, "head"),
        P(SLAB),
        P(SLAB, None),
        P(SLAB, None),
    )
    return jax.shard_map(
        per_device, mesh=finer, in_specs=placed, out_specs=P(None, SLAB, "head"), check_vma=False
    )
```

```python
import jax
import jax.numpy as jnp
from jax import lax
from jax.experimental import pallas as pl
from jax.experimental.layout import Layout, with_layout_constraint
from jax.experimental.pallas import tpu as pltpu
from jax.sharding import Mesh
from jax.sharding import PartitionSpec as P


SLAB = ("slab_0", "slab_1", "slab_2")
EMPTY = 2.0**127
WIDTH = 512
DEPTH = 2
SPILL = 5


def pack_kernel(turn, dest_ref, count_ref, rows_ref, out_ref, held, blank, seen, slot, in_sem, out_sem):
    slabs = out_ref.shape[0]
    parts = in_sem.shape[0]
    size = held.shape[0] // parts

    def fetch(p):
        part = pl.ds(p * size, size)
        return pltpu.make_async_copy(rows_ref.at[part], held.at[part], in_sem.at[p])

    for p in range(parts):
        fetch(p).start()
    blank[...] = jnp.full(blank.shape, EMPTY, blank.dtype)

    def clear(i, carry):
        seen[i] = 0
        return carry

    lax.fori_loop(0, slabs, clear, 0, unroll=8)
    live = count_ref[0]

    def number(r, carry):
        d = dest_ref[r]
        j = seen[d]
        seen[d] = j + 1
        slot[r] = jnp.where(j == turn, d, -1)
        return carry

    lax.fori_loop(0, live, number, 0)

    def leave(d, carry):
        @pl.when(seen[d] <= turn)
        def _():
            pltpu.make_async_copy(blank.at[0], out_ref.at[d], out_sem).start()

        return carry

    lax.fori_loop(0, slabs, leave, 0, unroll=4)
    for p in range(parts):
        fetch(p).wait()

    def send(r, carry):
        @pl.when(slot[r] >= 0)
        def _():
            pltpu.make_async_copy(held.at[r], out_ref.at[slot[r]], out_sem).start()

        return carry

    lax.fori_loop(0, live, send, 0)
    pltpu.make_async_copy(out_ref, out_ref, out_sem).wait()


def pack(outlier_rows, destinations, outlier_counts, slab_count, turn):
    row_slots, kinds, features = outlier_rows.shape
    smem = pl.BlockSpec(memory_space=pltpu.SMEM)
    anywhere = pl.BlockSpec(memory_space=pl.ANY)
    return pl.pallas_call(
        lambda *refs: pack_kernel(turn, *refs),
        name="pack",
        in_specs=[smem, smem, anywhere],
        out_specs=anywhere,
        out_shape=jax.ShapeDtypeStruct((slab_count, kinds, features), outlier_rows.dtype),
        scratch_shapes=[
            pltpu.VMEM(outlier_rows.shape, outlier_rows.dtype),
            pltpu.VMEM((1, kinds, features), outlier_rows.dtype),
            pltpu.SMEM((slab_count,), jnp.int32),
            pltpu.SMEM((row_slots,), jnp.int32),
            pltpu.SemaphoreType.DMA((4,)),
            pltpu.SemaphoreType.DMA,
        ],
        cost_estimate=pl.CostEstimate(
            flops=2000000, bytes_accessed=2 * row_slots * kinds * features * 2, transcendentals=0
        ),
    )(destinations[:, 0], outlier_counts, outlier_rows)


def spill_kernel(plane, dest_ref, count_ref, rows_ref, out_ref, seen, later, filled, mark, sem):
    planes = filled.shape[0]
    slabs = plane * planes
    places = out_ref.shape[0]
    cap = places // planes
    kinds = out_ref.shape[1]
    features = rows_ref.shape[2]

    def blank(i, carry):
        out_ref[i] = jnp.full(out_ref.shape[1:], EMPTY, out_ref.dtype)
        mark[i] = plane
        return carry

    lax.fori_loop(0, places, blank, 0)

    def clear(i, carry):
        seen[i] = 0
        return carry

    lax.fori_loop(0, slabs, clear, 0, unroll=8)
    seen[slabs] = 0
    for p in range(planes):
        filled[p] = 0
    live = count_ref[0]

    def number(r, found):
        d = jnp.where(r < live, dest_ref[r], slabs)
        j = seen[d]
        seen[d] = j + 1
        later[found] = r
        return found + jnp.where((j > 0) & (d < slabs), 1, 0)

    found = lax.fori_loop(0, dest_ref.shape[0], number, 0, unroll=8)

    def send(i, started):
        r = later[i]
        d = dest_ref[r]
        p = lax.div(d, plane)
        e = filled[p]
        filled[p] = e + 1

        @pl.when(e < cap)
        def _():
            at = p * cap + e
            mark[at] = d - p * plane
            pltpu.make_async_copy(
                rows_ref.at[r], out_ref.at[at, :, pl.ds(0, features)], sem
            ).start()

        return started + jnp.where(e < cap, 1, 0)

    started = lax.fori_loop(0, found, send, 0)
    most = filled[0]
    for p in range(1, planes):
        most = jnp.maximum(most, filled[p])
    over = jnp.where(most > cap, 2 * plane, 0)

    def label(i, carry):
        value = (mark[i] + over).astype(jnp.float32)
        out_ref[i, :, pl.ds(features, 128)] = jnp.full((kinds, 128), value).astype(out_ref.dtype)
        return carry

    lax.fori_loop(0, places, label, 0)

    def finish(r, carry):
        pltpu.make_async_copy(rows_ref.at[0], out_ref.at[0, :, pl.ds(0, features)], sem).wait()
        return carry

    lax.fori_loop(0, started, finish, 0)


def spill(outlier_rows, destinations, outlier_counts, slab_count, planes):
    _, kinds, features = outlier_rows.shape
    smem = pl.BlockSpec(memory_space=pltpu.SMEM)
    plane = slab_count // planes
    return pl.pallas_call(
        lambda *refs: spill_kernel(plane, *refs),
        name="spill",
        in_specs=[smem, smem, pl.BlockSpec(memory_space=pl.ANY)],
        out_specs=pl.BlockSpec(memory_space=pltpu.VMEM),
        out_shape=jax.ShapeDtypeStruct((planes * SPILL, kinds, features + 128), outlier_rows.dtype),
        scratch_shapes=[
            pltpu.SMEM((slab_count + 1,), jnp.int32),
            pltpu.SMEM((outlier_rows.shape[0] + 1,), jnp.int32),
            pltpu.SMEM((planes,), jnp.int32),
            pltpu.SMEM((planes * SPILL,), jnp.int32),
            pltpu.SemaphoreType.DMA,
        ],
        cost_estimate=pl.CostEstimate(
            flops=2000000, bytes_accessed=4 * planes * SPILL * kinds * features, transcendentals=0
        ),
    )(destinations[:, 0], outlier_counts, outlier_rows)


def relay_kernel(here_ref, in_ref, *out_refs):
    places, kinds, width = in_ref.shape
    count = len(out_refs)
    senders = out_refs[0].shape[0]
    cap = places // senders
    total = places * kinds
    lanes = 128
    rows = in_ref[...].reshape(total, width)
    labels = rows[:, width - lanes :]
    corner = jnp.where(lax.broadcasted_iota(jnp.int32, (8, lanes), 1) == 0, 1.0, 0.0).astype(jnp.bfloat16)
    over = (((1,), (1,)), ((), ()))
    label = lax.dot_general(corner, labels, over, preferred_element_type=jnp.float32)[0:1]
    label = label.astype(jnp.int32)
    full = jnp.max(label, axis=1, keepdims=True) >= 2 * count
    owner = label & (2 * count - 1)
    x, y = here_ref[0], here_ref[1]
    ahead = (((owner >> 2) - x) & 3) * 4 + (((owner & 3) - y) & 3)
    ahead = jnp.where(owner < count, ahead, count)
    part = senders * kinds
    source = lax.broadcasted_iota(jnp.int32, (count * part, total), 1)
    target = lax.broadcasted_iota(jnp.int32, (count * part, total), 0)
    same = source % kinds == target % kinds
    same &= source // (cap * kinds) == target // kinds % senders
    picked = jnp.where(same & (ahead == target // part), 1.0, 0.0)
    some = jnp.max(picked, axis=1, keepdims=True) > 0.5
    picker = picked.astype(jnp.bfloat16)
    step = 512
    for c in range(0, width - lanes, step):
        got = jnp.dot(picker, rows[:, c : c + step], preferred_element_type=jnp.float32)
        got = jnp.where(some, got, EMPTY).astype(in_ref.dtype)
        for o in range(count):
            out_refs[o][:, :, c : c + step] = got[o * part : (o + 1) * part].reshape(senders, kinds, step)
    told = jnp.where(full, 1.0, 0.0) * jnp.ones((part, lanes), jnp.float32)
    told = told.astype(in_ref.dtype).reshape(senders, kinds, lanes)
    for o in range(count):
        out_refs[o][:, :, width - lanes :] = told


def relay(gathered, here, planes, count):
    _, kinds, width = gathered.shape
    return pl.pallas_call(
        relay_kernel,
        name="relay",
        in_specs=[pl.BlockSpec(memory_space=pltpu.SMEM), pl.BlockSpec(memory_space=pltpu.VMEM)],
        out_specs=[pl.BlockSpec(memory_space=pltpu.VMEM)] * count,
        out_shape=[jax.ShapeDtypeStruct((planes, kinds, width), gathered.dtype)] * count,
        cost_estimate=pl.CostEstimate(
            flops=10000000, bytes_accessed=4 * count * planes * kinds * width, transcendentals=0
        ),
    )(here, gathered)


def prepare_kernel(dirs_ref, order_ref, out_ref, rank_ref):
    tokens = dirs_ref.shape[1]
    for v in range(2):
        ahead = pltpu.roll(dirs_ref[v].astype(jnp.float32), tokens - 1, 0)
        out_ref[v] = ahead.astype(out_ref.dtype)

    @pl.when(pl.program_id(0) == 0)
    def _():
        token = lax.broadcasted_iota(jnp.int32, (tokens, tokens), 0)
        number = lax.broadcasted_iota(jnp.int32, (tokens, tokens), 1)
        here = jnp.where(order_ref[...] == token, number, 0).astype(jnp.float32)
        rank = jnp.sum(here, axis=1, keepdims=True).astype(jnp.int32)
        rank_ref[...] = jnp.broadcast_to(rank, rank_ref.shape)


def prepare(directions, order):
    _, tokens, features = directions.shape
    width = 256
    spec = pl.BlockSpec((2, tokens, width), lambda i: (0, 0, i))
    return pl.pallas_call(
        prepare_kernel,
        name="prepare",
        compiler_params=pltpu.CompilerParams(vmem_limit_bytes=16 * 2**20),
        grid=(features // width,),
        in_specs=[spec, pl.BlockSpec((1, tokens), lambda i: (0, 0))],
        out_specs=[spec, pl.BlockSpec((tokens, 128), lambda i: (0, 0))],
        out_shape=[
            jax.ShapeDtypeStruct(directions.shape, directions.dtype),
            jax.ShapeDtypeStruct((tokens, 128), jnp.int32),
        ],
        cost_estimate=pl.CostEstimate(
            flops=20 * tokens * features, bytes_accessed=8 * tokens * features, transcendentals=0
        ),
    )(directions, order)


def place_kernel(
    first, second, order, rank, dirs, mags, edge, out,
    a_buf, k_buf, r_buf, d_buf, m_buf, e_buf, o_buf, placer, covered, wide,
    a_sem, k_sem, r_sem, d_sem, m_sem, e_sem, o_sem,
):
    blocks, kinds, tokens, width = o_buf.shape
    slots = a_buf.shape[1]
    half = slots // 2
    lanes = 128
    chunks = slots // lanes
    heads = width // lanes

    def columns(i):
        return pl.ds(pl.multiple_of(i * width, lanes), width)

    class a_copy:
        def __init__(self, i):
            self.parts = [
                pltpu.make_async_copy(
                    half_of.at[:, :, columns(i)], a_buf.at[i, pl.ds(j * half, half)], a_sem.at[i, j]
                )
                for j, half_of in enumerate((first, second))
            ]

        def start(self):
            for part in self.parts:
                part.start()

        def wait(self):
            for part in self.parts:
                part.wait()

    def d_copy(i):
        return pltpu.make_async_copy(dirs.at[:, :, columns(i)], d_buf.at[i], d_sem.at[i])

    def o_copy(i):
        return pltpu.make_async_copy(o_buf.at[i], out.at[:, :, columns(i)], o_sem.at[i])

    r_copy = pltpu.make_async_copy(rank, r_buf, r_sem)
    k_copy = pltpu.make_async_copy(order, k_buf, k_sem)
    m_copy = pltpu.make_async_copy(mags, m_buf, m_sem)
    e_copy = pltpu.make_async_copy(edge, e_buf, e_sem)
    a_copy(0).start()
    k_copy.start()
    r_copy.start()
    m_copy.start()
    e_copy.start()
    d_copy(0).start()
    for i in range(1, DEPTH):
        a_copy(i).start()
        d_copy(i).start()


    def block(i, carry):
        @pl.when(i + DEPTH < blocks)
        def _():
            a_copy(i + DEPTH).start()
            d_copy(i + DEPTH).start()

        a_copy(i).wait()
        for c in range(heads):
            wide[c] = (
                a_buf[i, :, :, c * lanes : (c + 1) * lanes]
                .reshape(slots * kinds, lanes)
                .astype(jnp.float32)
            )

        @pl.when(i == 0)
        def _():
            corner_of = wide[0, pl.ds(0, slots, stride=kinds), :]
            full = jnp.where(corner_of < EMPTY, 1.0, 0.0).astype(jnp.bfloat16)
            corner = jnp.where(lax.broadcasted_iota(jnp.int32, (8, lanes), 1) == 0, 1.0, 0.0)
            corner = corner.astype(jnp.bfloat16)
            over = (((1,), (1,)), ((), ()))
            filled = [
                lax.dot_general(
                    corner, full[c * lanes : (c + 1) * lanes], over, preferred_element_type=jnp.float32
                )
                for c in range(chunks)
            ]
            run = jnp.sum(sum(filled), axis=1, keepdims=True)[0:1]
            k_copy.wait()
            ahead = []
            for c in range(chunks):
                number = jnp.zeros((8, lanes), jnp.float32)
                for e in range(chunks):
                    earlier = k_buf[e, :, :] < k_buf[2 + c, 0:1, :]
                    number += jnp.dot(
                        filled[e].astype(jnp.bfloat16),
                        jnp.where(earlier, 1.0, 0.0).astype(jnp.bfloat16),
                        preferred_element_type=jnp.float32,
                    )
                ahead.append(jnp.where(filled[c] > 0.5, number, -1.0).astype(jnp.int32))
            r_copy.wait()
            m_copy.wait()
            e_copy.wait()
            place_of = r_buf[...]
            covered[...] = jnp.where(place_of < run.astype(jnp.int32), 1, 0)
            for c in range(chunks):
                placer[:, c * lanes : (c + 1) * lanes] = jnp.where(
                    place_of == ahead[c][0:1], 1.0, 0.0
                ).astype(jnp.bfloat16)

        d_copy(i).wait()
        tail = slice(tokens - 16, tokens)
        last = lax.broadcasted_iota(jnp.int32, (16, width), 0) == 15
        for v in range(2):
            end = d_buf[i, v, tail].astype(jnp.float32)
            end = jnp.where(last, e_buf[v : v + 1, columns(i)], end)
            d_buf[i, v, tail] = end.astype(d_buf.dtype)
        given = e_buf[2:3, pl.ds(pl.multiple_of(i * lanes, lanes), lanes)]
        m_buf[i, tail] = jnp.where(last[:, 0:lanes], given, m_buf[i, tail])
        factors = jnp.where(covered[...] > 0, 0.0, m_buf[i])
        own_dirs = [d_buf[i, v].astype(jnp.float32) for v in range(2)]
        for k in range(kinds):
          for c0 in range(0, heads, 2):
            rows = jnp.concatenate(
                [wide[c, pl.ds(k, slots, stride=kinds), :] for c in range(c0, c0 + 2)], axis=1
            ).astype(jnp.bfloat16)
            both = jnp.dot(placer[...], rows, preferred_element_type=jnp.float32)
            for c in range(c0, c0 + 2):
                part = slice(c * lanes, (c + 1) * lanes)
                got = both[:, (c - c0) * lanes : (c - c0 + 1) * lanes]
                own = factors[:, k * heads + c : k * heads + c + 1] * own_dirs[k % 2][:, part]
                o_buf[i, k, :, part] = (got + own).astype(o_buf.dtype)
        o_copy(i).start()
        return carry

    lax.fori_loop(0, blocks, block, 0)
    for i in range(blocks):
        o_copy(i).wait()


def place(first, second, order, rank, dirs, mags, edge):
    slabs, kinds, features = first.shape
    slots = 2 * slabs
    _, tokens, _ = dirs.shape
    width = WIDTH
    blocks = features // width
    anywhere = pl.BlockSpec(memory_space=pl.ANY)
    return pl.pallas_call(
        place_kernel,
        name="place",
        in_specs=[anywhere] * 7,
        out_specs=anywhere,
        out_shape=jax.ShapeDtypeStruct((kinds, tokens, features), first.dtype),
        scratch_shapes=[
            pltpu.VMEM((blocks, slots, kinds, width), first.dtype),
            pltpu.VMEM(order.shape, order.dtype),
            pltpu.VMEM(rank.shape, rank.dtype),
            pltpu.VMEM((blocks, 2, tokens, width), dirs.dtype),
            pltpu.VMEM(mags.shape, mags.dtype),
            pltpu.VMEM(edge.shape, edge.dtype),
            pltpu.VMEM((blocks, kinds, tokens, width), first.dtype),
            pltpu.VMEM((tokens, slots), jnp.bfloat16),
            pltpu.VMEM((tokens, 128), jnp.int32),
            pltpu.VMEM((width // 128, slots * kinds, 128), jnp.float32),
            pltpu.SemaphoreType.DMA((blocks, 2)),
            pltpu.SemaphoreType.DMA,
            pltpu.SemaphoreType.DMA,
            pltpu.SemaphoreType.DMA((blocks,)),
            pltpu.SemaphoreType.DMA,
            pltpu.SemaphoreType.DMA,
            pltpu.SemaphoreType.DMA((blocks,)),
        ],
        cost_estimate=pl.CostEstimate(
            flops=2 * kinds * tokens * slots * features,
            bytes_accessed=2 * (slots * kinds + 2 * tokens + kinds * tokens) * features,
            transcendentals=0,
        ),
    )(first, second, order, rank, dirs, mags, edge)


def passed_back(block, axis):
    devices = lax.axis_size(axis)
    return lax.ppermute(block, axis, [((i + 1) % devices, i) for i in range(devices)])


def per_device(directions, magnitudes, outlier_rows, outlier_counts, destinations, retention_order):
    slab_count = lax.axis_size(SLAB)
    features = directions.shape[2]
    heads = magnitudes.shape[1]
    planes = lax.axis_size("slab_0")
    plane = ("slab_1", "slab_2")
    wide, deep = lax.axis_size("slab_1"), lax.axis_size("slab_2")
    x, y = lax.axis_index("slab_1"), lax.axis_index("slab_2")

    spilled = spill(outlier_rows, destinations, outlier_counts, slab_count, planes)
    gathered = lax.all_to_all(spilled, "slab_0", split_axis=0, concat_axis=0, tiled=True)
    packed = pack(outlier_rows, destinations, outlier_counts, slab_count, 0)
    packed, gathered = lax.optimization_barrier((packed, gathered))
    first = lax.all_to_all(packed, SLAB, split_axis=0, concat_axis=0, tiled=True)

    sorted_rows = relay(gathered, jnp.stack([x, y]).astype(jnp.int32), planes, wide * deep)
    steps = [(dx, dy) for dx in range(wide) for dy in range(deep)]
    second = []
    for (dx, dy), rows in zip(steps, sorted_rows):
        if (dx, dy) != (0, 0):
            route = [
                (i * deep + j, (i + dx) % wide * deep + (j + dy) % deep)
                for i in range(wide)
                for j in range(deep)
            ]
            rows = lax.ppermute(rows, plane, route)
        second.append(rows)
    second = jnp.concatenate(second, axis=0)
    too_many = jnp.max(second[:, 0, features]) > 0.5

    slabs = jnp.arange(slab_count, dtype=jnp.int32)
    step, z = slabs // planes, slabs % planes
    came = z * (wide * deep) + (x - step // deep) % wide * deep + (y - step % deep) % deep

    def order_of(first_slab, second_slab):
        keys = jnp.stack([2 * first_slab, 2 * second_slab + 1]).astype(jnp.int32)
        return jnp.concatenate(
            [
                jnp.broadcast_to(keys[:, :, None], (2, slab_count, 128)),
                jnp.broadcast_to(keys[:, None, :], (2, slab_count, 128)),
            ]
        )

    blocks = features // WIDTH

    def by_block(block):
        count = block.shape[2]
        block = block.reshape(4, blocks, heads // blocks, count).transpose(1, 3, 0, 2)
        block = block.reshape(blocks, count, 4 * heads // blocks)
        return jnp.pad(block, ((0, 0), (0, 0), (0, 128 - block.shape[2])))

    first_mags = by_block(magnitudes[:, :, :1]).reshape(1, blocks * 128)
    edge = jnp.concatenate(
        [
            directions[:, 0, :].astype(jnp.float32),
            jnp.pad(first_mags, ((0, 1), (0, features - blocks * 128))),
        ]
    )
    edge = passed_back(edge, SLAB)
    factors = by_block(jnp.roll(magnitudes, -1, axis=2))
    factors = with_layout_constraint(factors, Layout(major_to_minor=(0, 1, 2)))
    dirs, rank = prepare(directions, retention_order)
    relayed, direct = order_of(slabs, came), order_of(slabs, slabs)

    def short(_):
        return place(first, second, relayed, rank, dirs, factors, edge)

    def long(_):
        rest = pack(outlier_rows, destinations, outlier_counts, slab_count, 1)
        rest = lax.all_to_all(rest, SLAB, split_axis=0, concat_axis=0, tiled=True)
        return place(first, rest, direct, rank, dirs, factors, edge)

    return lax.cond(too_many, long, short, 0)


def solution(mesh):
    finer = Mesh(
        mesh.devices.reshape(8, 4, 4, mesh.shape["head"]), ("slab_0", "slab_1", "slab_2", "head")
    )
    placed = (
        P(None, SLAB, "head"),
        P(None, "head", SLAB),
        P(SLAB, None, "head"),
        P(SLAB),
        P(SLAB, None),
        P(SLAB, None),
    )
    return jax.shard_map(
        per_device, mesh=finer, in_specs=placed, out_specs=P(None, SLAB, "head"), check_vma=False
    )
```

```python
import jax
import jax.numpy as jnp
from jax import lax
from jax.experimental import pallas as pl
from jax.experimental.layout import Layout, with_layout_constraint
from jax.experimental.pallas import tpu as pltpu
from jax.sharding import Mesh
from jax.sharding import PartitionSpec as P


SLAB = ("slab_0", "slab_1", "slab_2")
EMPTY = 2.0**127
WIDTH = 512
DEPTH = 2
SPILL = 5


def pack_kernel(turn, dest_ref, count_ref, rows_ref, out_ref, held, blank, seen, slot, in_sem, out_sem):
    slabs = out_ref.shape[0]
    parts = in_sem.shape[0]
    size = held.shape[0] // parts

    def fetch(p):
        part = pl.ds(p * size, size)
        return pltpu.make_async_copy(rows_ref.at[part], held.at[part], in_sem.at[p])

    for p in range(parts):
        fetch(p).start()
    blank[...] = jnp.full(blank.shape, EMPTY, blank.dtype)

    def clear(i, carry):
        seen[i] = 0
        return carry

    lax.fori_loop(0, slabs, clear, 0, unroll=8)
    live = count_ref[0]

    def number(r, carry):
        d = dest_ref[r]
        j = seen[d]
        seen[d] = j + 1
        slot[r] = jnp.where(j == turn, d, -1)
        return carry

    lax.fori_loop(0, live, number, 0)

    def leave(d, carry):
        @pl.when(seen[d] <= turn)
        def _():
            pltpu.make_async_copy(blank.at[0], out_ref.at[d], out_sem).start()

        return carry

    lax.fori_loop(0, slabs, leave, 0, unroll=4)
    for p in range(parts):
        fetch(p).wait()

    def send(r, carry):
        @pl.when(slot[r] >= 0)
        def _():
            pltpu.make_async_copy(held.at[r], out_ref.at[slot[r]], out_sem).start()

        return carry

    lax.fori_loop(0, live, send, 0)
    pltpu.make_async_copy(out_ref, out_ref, out_sem).wait()


def pack(outlier_rows, destinations, outlier_counts, slab_count, turn):
    row_slots, kinds, features = outlier_rows.shape
    smem = pl.BlockSpec(memory_space=pltpu.SMEM)
    anywhere = pl.BlockSpec(memory_space=pl.ANY)
    return pl.pallas_call(
        lambda *refs: pack_kernel(turn, *refs),
        name="pack",
        in_specs=[smem, smem, anywhere],
        out_specs=anywhere,
        out_shape=jax.ShapeDtypeStruct((slab_count, kinds, features), outlier_rows.dtype),
        scratch_shapes=[
            pltpu.VMEM(outlier_rows.shape, outlier_rows.dtype),
            pltpu.VMEM((1, kinds, features), outlier_rows.dtype),
            pltpu.SMEM((slab_count,), jnp.int32),
            pltpu.SMEM((row_slots,), jnp.int32),
            pltpu.SemaphoreType.DMA((4,)),
            pltpu.SemaphoreType.DMA,
        ],
        cost_estimate=pl.CostEstimate(
            flops=2000000, bytes_accessed=2 * row_slots * kinds * features * 2, transcendentals=0
        ),
    )(destinations[:, 0], outlier_counts, outlier_rows)


def spill_kernel(plane, dest_ref, count_ref, rows_ref, out_ref, seen, later, filled, mark, sem):
    planes = filled.shape[0]
    slabs = plane * planes
    places = out_ref.shape[0]
    cap = places // planes
    kinds = out_ref.shape[1]
    features = rows_ref.shape[2]

    def blank(i, carry):
        out_ref[i] = jnp.full(out_ref.shape[1:], EMPTY, out_ref.dtype)
        mark[i] = plane
        return carry

    lax.fori_loop(0, places, blank, 0)

    def clear(i, carry):
        seen[i] = 0
        return carry

    lax.fori_loop(0, slabs, clear, 0, unroll=8)
    seen[slabs] = 0
    for p in range(planes):
        filled[p] = 0
    live = count_ref[0]

    def number(r, found):
        d = jnp.where(r < live, dest_ref[r], slabs)
        j = seen[d]
        seen[d] = j + 1
        later[found] = r
        return found + jnp.where((j > 0) & (d < slabs), 1, 0)

    found = lax.fori_loop(0, dest_ref.shape[0], number, 0, unroll=8)

    def send(i, started):
        r = later[i]
        d = dest_ref[r]
        p = lax.div(d, plane)
        e = filled[p]
        filled[p] = e + 1

        @pl.when(e < cap)
        def _():
            at = p * cap + e
            mark[at] = d - p * plane
            pltpu.make_async_copy(
                rows_ref.at[r], out_ref.at[at, :, pl.ds(0, features)], sem
            ).start()

        return started + jnp.where(e < cap, 1, 0)

    started = lax.fori_loop(0, found, send, 0)
    most = filled[0]
    for p in range(1, planes):
        most = jnp.maximum(most, filled[p])
    over = jnp.where(most > cap, 2 * plane, 0)

    def label(i, carry):
        value = (mark[i] + over).astype(jnp.float32)
        out_ref[i, :, pl.ds(features, 128)] = jnp.full((kinds, 128), value).astype(out_ref.dtype)
        return carry

    lax.fori_loop(0, places, label, 0)

    def finish(r, carry):
        pltpu.make_async_copy(rows_ref.at[0], out_ref.at[0, :, pl.ds(0, features)], sem).wait()
        return carry

    lax.fori_loop(0, started, finish, 0)


def spill(outlier_rows, destinations, outlier_counts, slab_count, planes):
    _, kinds, features = outlier_rows.shape
    smem = pl.BlockSpec(memory_space=pltpu.SMEM)
    plane = slab_count // planes
    return pl.pallas_call(
        lambda *refs: spill_kernel(plane, *refs),
        name="spill",
        in_specs=[smem, smem, pl.BlockSpec(memory_space=pl.ANY)],
        out_specs=pl.BlockSpec(memory_space=pltpu.VMEM),
        out_shape=jax.ShapeDtypeStruct((planes * SPILL, kinds, features + 128), outlier_rows.dtype),
        scratch_shapes=[
            pltpu.SMEM((slab_count + 1,), jnp.int32),
            pltpu.SMEM((outlier_rows.shape[0] + 1,), jnp.int32),
            pltpu.SMEM((planes,), jnp.int32),
            pltpu.SMEM((planes * SPILL,), jnp.int32),
            pltpu.SemaphoreType.DMA,
        ],
        cost_estimate=pl.CostEstimate(
            flops=2000000, bytes_accessed=4 * planes * SPILL * kinds * features, transcendentals=0
        ),
    )(destinations[:, 0], outlier_counts, outlier_rows)


def relay_kernel(here_ref, in_ref, *out_refs):
    places, kinds, width = in_ref.shape
    count = len(out_refs)
    senders = out_refs[0].shape[0] // kinds
    cap = places // senders
    total = places * kinds
    lanes = 128
    rows = in_ref[...].reshape(total, width)
    labels = rows[:, width - lanes :]
    corner = jnp.where(lax.broadcasted_iota(jnp.int32, (8, lanes), 1) == 0, 1.0, 0.0).astype(jnp.bfloat16)
    over = (((1,), (1,)), ((), ()))
    label = lax.dot_general(corner, labels, over, preferred_element_type=jnp.float32)[0:1]
    label = label.astype(jnp.int32)
    full = jnp.max(label, axis=1, keepdims=True) >= 2 * count
    owner = label & (2 * count - 1)
    x, y = here_ref[0], here_ref[1]
    ahead = (((owner >> 2) - x) & 3) * 4 + (((owner & 3) - y) & 3)
    ahead = jnp.where(owner < count, ahead, count)
    part = senders * kinds
    source = lax.broadcasted_iota(jnp.int32, (count * part, total), 1)
    target = lax.broadcasted_iota(jnp.int32, (count * part, total), 0)
    same = source % kinds == target % kinds
    same &= source // (cap * kinds) == target // kinds % senders
    picked = jnp.where(same & (ahead == target // part), 1.0, 0.0)
    some = jnp.max(picked, axis=1, keepdims=True) > 0.5
    picker = picked.astype(jnp.bfloat16)
    step = 512
    for c in range(0, width - lanes, step):
        got = jnp.dot(picker, rows[:, c : c + step], preferred_element_type=jnp.float32)
        got = jnp.where(some, got, EMPTY).astype(in_ref.dtype)
        for o in range(count):
            out_refs[o][:, c : c + step] = got[o * part : (o + 1) * part]
    told = jnp.where(full, 1.0, 0.0) * jnp.ones((part, lanes), jnp.float32)
    told = told.astype(in_ref.dtype)
    for o in range(count):
        out_refs[o][:, width - lanes :] = told


def relay(gathered, here, planes, count):
    _, kinds, width = gathered.shape
    return pl.pallas_call(
        relay_kernel,
        name="relay",
        in_specs=[pl.BlockSpec(memory_space=pltpu.SMEM), pl.BlockSpec(memory_space=pltpu.VMEM)],
        out_specs=[pl.BlockSpec(memory_space=pltpu.VMEM)] * count,
        out_shape=[jax.ShapeDtypeStruct((planes * kinds, width), gathered.dtype)] * count,
        cost_estimate=pl.CostEstimate(
            flops=10000000, bytes_accessed=4 * count * planes * kinds * width, transcendentals=0
        ),
    )(here, gathered)


def prepare_kernel(dirs_ref, order_ref, out_ref, rank_ref):
    tokens = dirs_ref.shape[1]
    for v in range(2):
        ahead = pltpu.roll(dirs_ref[v].astype(jnp.float32), tokens - 1, 0)
        out_ref[v] = ahead.astype(out_ref.dtype)

    @pl.when(pl.program_id(0) == 0)
    def _():
        token = lax.broadcasted_iota(jnp.int32, (tokens, tokens), 0)
        number = lax.broadcasted_iota(jnp.int32, (tokens, tokens), 1)
        here = jnp.where(order_ref[...] == token, number, 0).astype(jnp.float32)
        rank = jnp.sum(here, axis=1, keepdims=True).astype(jnp.int32)
        rank_ref[...] = jnp.broadcast_to(rank, rank_ref.shape)


def prepare(directions, order):
    _, tokens, features = directions.shape
    width = 256
    spec = pl.BlockSpec((2, tokens, width), lambda i: (0, 0, i))
    return pl.pallas_call(
        prepare_kernel,
        name="prepare",
        compiler_params=pltpu.CompilerParams(vmem_limit_bytes=16 * 2**20),
        grid=(features // width,),
        in_specs=[spec, pl.BlockSpec((1, tokens), lambda i: (0, 0))],
        out_specs=[spec, pl.BlockSpec((tokens, 128), lambda i: (0, 0))],
        out_shape=[
            jax.ShapeDtypeStruct(directions.shape, directions.dtype),
            jax.ShapeDtypeStruct((tokens, 128), jnp.int32),
        ],
        cost_estimate=pl.CostEstimate(
            flops=20 * tokens * features, bytes_accessed=8 * tokens * features, transcendentals=0
        ),
    )(directions, order)


def place_kernel(
    first, second, order, rank, dirs, mags, edge, out,
    a_buf, b_buf, k_buf, r_buf, d_buf, m_buf, e_buf, o_buf, placer, covered, wide,
    a_sem, k_sem, r_sem, d_sem, m_sem, e_sem, o_sem,
):
    blocks, kinds, tokens, width = o_buf.shape
    half = a_buf.shape[1]
    slots = 2 * half
    lanes = 128
    chunks = slots // lanes
    heads = width // lanes

    def columns(i):
        return pl.ds(pl.multiple_of(i * width, lanes), width)

    class a_copy:
        def __init__(self, i):
            self.parts = (
                pltpu.make_async_copy(first.at[:, :, columns(i)], a_buf.at[i], a_sem.at[i, 0]),
                pltpu.make_async_copy(second.at[:, columns(i)], b_buf.at[i], a_sem.at[i, 1]),
            )

        def start(self):
            for part in self.parts:
                part.start()

        def wait(self):
            for part in self.parts:
                part.wait()

    def d_copy(i):
        return pltpu.make_async_copy(dirs.at[:, :, columns(i)], d_buf.at[i], d_sem.at[i])

    def o_copy(i):
        return pltpu.make_async_copy(o_buf.at[i], out.at[:, :, columns(i)], o_sem.at[i])

    r_copy = pltpu.make_async_copy(rank, r_buf, r_sem)
    k_copy = pltpu.make_async_copy(order, k_buf, k_sem)
    m_copy = pltpu.make_async_copy(mags, m_buf, m_sem)
    e_copy = pltpu.make_async_copy(edge, e_buf, e_sem)
    a_copy(0).start()
    k_copy.start()
    r_copy.start()
    m_copy.start()
    e_copy.start()
    d_copy(0).start()
    for i in range(1, DEPTH):
        a_copy(i).start()
        d_copy(i).start()


    def block(i, carry):
        @pl.when(i + DEPTH < blocks)
        def _():
            a_copy(i + DEPTH).start()
            d_copy(i + DEPTH).start()

        a_copy(i).wait()
        for c in range(heads):
            part = slice(c * lanes, (c + 1) * lanes)
            wide[c, : half * kinds] = (
                a_buf[i, :, :, part].reshape(half * kinds, lanes).astype(jnp.float32)
            )
            wide[c, half * kinds :] = b_buf[i, :, part].astype(jnp.float32)

        @pl.when(i == 0)
        def _():
            corner_of = wide[0, pl.ds(0, slots, stride=kinds), :]
            full = jnp.where(corner_of < EMPTY, 1.0, 0.0).astype(jnp.bfloat16)
            corner = jnp.where(lax.broadcasted_iota(jnp.int32, (8, lanes), 1) == 0, 1.0, 0.0)
            corner = corner.astype(jnp.bfloat16)
            over = (((1,), (1,)), ((), ()))
            filled = [
                lax.dot_general(
                    corner, full[c * lanes : (c + 1) * lanes], over, preferred_element_type=jnp.float32
                )
                for c in range(chunks)
            ]
            run = jnp.sum(sum(filled), axis=1, keepdims=True)[0:1]
            k_copy.wait()
            ahead = []
            for c in range(chunks):
                number = jnp.zeros((8, lanes), jnp.float32)
                for e in range(chunks):
                    earlier = k_buf[e, :, :] < k_buf[2 + c, 0:1, :]
                    number += jnp.dot(
                        filled[e].astype(jnp.bfloat16),
                        jnp.where(earlier, 1.0, 0.0).astype(jnp.bfloat16),
                        preferred_element_type=jnp.float32,
                    )
                ahead.append(jnp.where(filled[c] > 0.5, number, -1.0).astype(jnp.int32))
            r_copy.wait()
            m_copy.wait()
            e_copy.wait()
            place_of = r_buf[...]
            covered[...] = jnp.where(place_of < run.astype(jnp.int32), 1, 0)
            for c in range(chunks):
                placer[:, c * lanes : (c + 1) * lanes] = jnp.where(
                    place_of == ahead[c][0:1], 1.0, 0.0
                ).astype(jnp.bfloat16)

        d_copy(i).wait()
        tail = slice(tokens - 16, tokens)
        last = lax.broadcasted_iota(jnp.int32, (16, width), 0) == 15
        for v in range(2):
            end = d_buf[i, v, tail].astype(jnp.float32)
            end = jnp.where(last, e_buf[v : v + 1, columns(i)], end)
            d_buf[i, v, tail] = end.astype(d_buf.dtype)
        given = e_buf[2:3, pl.ds(pl.multiple_of(i * lanes, lanes), lanes)]
        m_buf[i, tail] = jnp.where(last[:, 0:lanes], given, m_buf[i, tail])
        factors = jnp.where(covered[...] > 0, 0.0, m_buf[i])
        own_dirs = [d_buf[i, v].astype(jnp.float32) for v in range(2)]
        for k in range(kinds):
          for c0 in range(0, heads, 2):
            rows = jnp.concatenate(
                [wide[c, pl.ds(k, slots, stride=kinds), :] for c in range(c0, c0 + 2)], axis=1
            ).astype(jnp.bfloat16)
            both = jnp.dot(placer[...], rows, preferred_element_type=jnp.float32)
            for c in range(c0, c0 + 2):
                part = slice(c * lanes, (c + 1) * lanes)
                got = both[:, (c - c0) * lanes : (c - c0 + 1) * lanes]
                own = factors[:, k * heads + c : k * heads + c + 1] * own_dirs[k % 2][:, part]
                o_buf[i, k, :, part] = (got + own).astype(o_buf.dtype)
        o_copy(i).start()
        return carry

    lax.fori_loop(0, blocks, block, 0)
    for i in range(blocks):
        o_copy(i).wait()


def place(first, second, order, rank, dirs, mags, edge):
    slabs, kinds, features = first.shape
    slots = 2 * slabs
    _, tokens, _ = dirs.shape
    width = WIDTH
    blocks = features // width
    anywhere = pl.BlockSpec(memory_space=pl.ANY)
    return pl.pallas_call(
        place_kernel,
        name="place",
        in_specs=[anywhere] * 7,
        out_specs=anywhere,
        out_shape=jax.ShapeDtypeStruct((kinds, tokens, features), first.dtype),
        scratch_shapes=[
            pltpu.VMEM((blocks, slabs, kinds, width), first.dtype),
            pltpu.VMEM((blocks, slabs * kinds, width), first.dtype),
            pltpu.VMEM(order.shape, order.dtype),
            pltpu.VMEM(rank.shape, rank.dtype),
            pltpu.VMEM((blocks, 2, tokens, width), dirs.dtype),
            pltpu.VMEM(mags.shape, mags.dtype),
            pltpu.VMEM(edge.shape, edge.dtype),
            pltpu.VMEM((blocks, kinds, tokens, width), first.dtype),
            pltpu.VMEM((tokens, slots), jnp.bfloat16),
            pltpu.VMEM((tokens, 128), jnp.int32),
            pltpu.VMEM((width // 128, slots * kinds, 128), jnp.float32),
            pltpu.SemaphoreType.DMA((blocks, 2)),
            pltpu.SemaphoreType.DMA,
            pltpu.SemaphoreType.DMA,
            pltpu.SemaphoreType.DMA((blocks,)),
            pltpu.SemaphoreType.DMA,
            pltpu.SemaphoreType.DMA,
            pltpu.SemaphoreType.DMA((blocks,)),
        ],
        cost_estimate=pl.CostEstimate(
            flops=2 * kinds * tokens * slots * features,
            bytes_accessed=2 * (slots * kinds + 2 * tokens + kinds * tokens) * features,
            transcendentals=0,
        ),
    )(first, second, order, rank, dirs, mags, edge)


def passed_back(block, axis):
    devices = lax.axis_size(axis)
    return lax.ppermute(block, axis, [((i + 1) % devices, i) for i in range(devices)])


def per_device(directions, magnitudes, outlier_rows, outlier_counts, destinations, retention_order):
    slab_count = lax.axis_size(SLAB)
    features = directions.shape[2]
    heads = magnitudes.shape[1]
    planes = lax.axis_size("slab_0")
    plane = ("slab_1", "slab_2")
    wide, deep = lax.axis_size("slab_1"), lax.axis_size("slab_2")
    x, y = lax.axis_index("slab_1"), lax.axis_index("slab_2")

    spilled = spill(outlier_rows, destinations, outlier_counts, slab_count, planes)
    gathered = lax.all_to_all(spilled, "slab_0", split_axis=0, concat_axis=0, tiled=True)
    packed = pack(outlier_rows, destinations, outlier_counts, slab_count, 0)
    packed, gathered = lax.optimization_barrier((packed, gathered))
    first = lax.all_to_all(packed, SLAB, split_axis=0, concat_axis=0, tiled=True)

    sorted_rows = relay(gathered, jnp.stack([x, y]).astype(jnp.int32), planes, wide * deep)
    steps = [(dx, dy) for dx in range(wide) for dy in range(deep)]
    second = []
    for (dx, dy), rows in zip(steps, sorted_rows):
        if (dx, dy) != (0, 0):
            route = [
                (i * deep + j, (i + dx) % wide * deep + (j + dy) % deep)
                for i in range(wide)
                for j in range(deep)
            ]
            rows = lax.ppermute(rows, plane, route)
        second.append(rows)
    second = jnp.concatenate(second, axis=0)
    too_many = jnp.max(second[:, features]) > 0.5

    slabs = jnp.arange(slab_count, dtype=jnp.int32)
    step, z = slabs // planes, slabs % planes
    came = z * (wide * deep) + (x - step // deep) % wide * deep + (y - step % deep) % deep

    def order_of(first_slab, second_slab):
        keys = jnp.stack([2 * first_slab, 2 * second_slab + 1]).astype(jnp.int32)
        return jnp.concatenate(
            [
                jnp.broadcast_to(keys[:, :, None], (2, slab_count, 128)),
                jnp.broadcast_to(keys[:, None, :], (2, slab_count, 128)),
            ]
        )

    blocks = features // WIDTH

    def by_block(block):
        count = block.shape[2]
        block = block.reshape(4, blocks, heads // blocks, count).transpose(1, 3, 0, 2)
        block = block.reshape(blocks, count, 4 * heads // blocks)
        return jnp.pad(block, ((0, 0), (0, 0), (0, 128 - block.shape[2])))

    first_mags = by_block(magnitudes[:, :, :1]).reshape(1, blocks * 128)
    edge = jnp.concatenate(
        [
            directions[:, 0, :].astype(jnp.float32),
            jnp.pad(first_mags, ((0, 1), (0, features - blocks * 128))),
        ]
    )
    edge = passed_back(edge, SLAB)
    factors = by_block(jnp.roll(magnitudes, -1, axis=2))
    factors = with_layout_constraint(factors, Layout(major_to_minor=(0, 1, 2)))
    dirs, rank = prepare(directions, retention_order)
    relayed, direct = order_of(slabs, came), order_of(slabs, slabs)

    def short(_):
        return place(first, second, relayed, rank, dirs, factors, edge)

    def long(_):
        rest = pack(outlier_rows, destinations, outlier_counts, slab_count, 1)
        rest = lax.all_to_all(rest, SLAB, split_axis=0, concat_axis=0, tiled=True)
        rest = rest.reshape(-1, features)
        return place(first, rest, direct, rank, dirs, factors, edge)

    return lax.cond(too_many, long, short, 0)


def solution(mesh):
    finer = Mesh(
        mesh.devices.reshape(8, 4, 4, mesh.shape["head"]), ("slab_0", "slab_1", "slab_2", "head")
    )
    placed = (
        P(None, SLAB, "head"),
        P(None, "head", SLAB),
        P(SLAB, None, "head"),
        P(SLAB),
        P(SLAB, None),
        P(SLAB, None),
    )
    return jax.shard_map(
        per_device, mesh=finer, in_specs=placed, out_specs=P(None, SLAB, "head"), check_vma=False
    )
```

```python
import functools

import jax
import jax.numpy as jnp
from jax import lax
from jax.experimental import pallas as pl
from jax.experimental.layout import Layout, with_layout_constraint
from jax.experimental.pallas import tpu as pltpu
from jax.sharding import Mesh
from jax.sharding import PartitionSpec as P


SLAB = ("slab_0", "slab_1", "slab_2")
EMPTY = 2.0**127
WIDTH = 512
DEPTH = 2
SPILL = 5


def pack_kernel(turn, dest_ref, count_ref, rows_ref, out_ref, held, blank, seen, slot, in_sem, out_sem):
    slabs = out_ref.shape[0]
    parts = in_sem.shape[0]
    size = held.shape[0] // parts

    def fetch(p):
        part = pl.ds(p * size, size)
        return pltpu.make_async_copy(rows_ref.at[part], held.at[part], in_sem.at[p])

    for p in range(parts):
        fetch(p).start()
    blank[...] = jnp.full(blank.shape, EMPTY, blank.dtype)

    def clear(i, carry):
        seen[i] = 0
        return carry

    lax.fori_loop(0, slabs, clear, 0, unroll=8)
    live = count_ref[0]

    def number(r, carry):
        d = dest_ref[r]
        j = seen[d]
        seen[d] = j + 1
        slot[r] = jnp.where(j == turn, d, -1)
        return carry

    lax.fori_loop(0, live, number, 0)

    def leave(d, carry):
        @pl.when(seen[d] <= turn)
        def _():
            pltpu.make_async_copy(blank.at[0], out_ref.at[d], out_sem).start()

        return carry

    lax.fori_loop(0, slabs, leave, 0, unroll=4)
    for p in range(parts):
        fetch(p).wait()

    def send(r, carry):
        @pl.when(slot[r] >= 0)
        def _():
            pltpu.make_async_copy(held.at[r], out_ref.at[slot[r]], out_sem).start()

        return carry

    lax.fori_loop(0, live, send, 0)
    pltpu.make_async_copy(out_ref, out_ref, out_sem).wait()


def pack(outlier_rows, destinations, outlier_counts, slab_count, turn):
    row_slots, kinds, features = outlier_rows.shape
    smem = pl.BlockSpec(memory_space=pltpu.SMEM)
    anywhere = pl.BlockSpec(memory_space=pl.ANY)
    return pl.pallas_call(
        lambda *refs: pack_kernel(turn, *refs),
        name="pack",
        in_specs=[smem, smem, anywhere],
        out_specs=anywhere,
        out_shape=jax.ShapeDtypeStruct((slab_count, kinds, features), outlier_rows.dtype),
        scratch_shapes=[
            pltpu.VMEM(outlier_rows.shape, outlier_rows.dtype),
            pltpu.VMEM((1, kinds, features), outlier_rows.dtype),
            pltpu.SMEM((slab_count,), jnp.int32),
            pltpu.SMEM((row_slots,), jnp.int32),
            pltpu.SemaphoreType.DMA((4,)),
            pltpu.SemaphoreType.DMA,
        ],
        cost_estimate=pl.CostEstimate(
            flops=2000000, bytes_accessed=2 * row_slots * kinds * features * 2, transcendentals=0
        ),
    )(destinations[:, 0], outlier_counts, outlier_rows)


def spill_kernel(plane, dest_ref, count_ref, rows_ref, out_ref, seen, later, filled, mark, sem):
    planes = filled.shape[0]
    slabs = plane * planes
    places = out_ref.shape[0]
    cap = places // planes
    kinds = out_ref.shape[1]
    features = rows_ref.shape[2]

    def blank(i, carry):
        out_ref[i] = jnp.full(out_ref.shape[1:], EMPTY, out_ref.dtype)
        mark[i] = plane
        return carry

    lax.fori_loop(0, places, blank, 0)

    def clear(i, carry):
        seen[i] = 0
        return carry

    lax.fori_loop(0, slabs, clear, 0, unroll=8)
    seen[slabs] = 0
    for p in range(planes):
        filled[p] = 0
    live = count_ref[0]

    def number(r, found):
        d = jnp.where(r < live, dest_ref[r], slabs)
        j = seen[d]
        seen[d] = j + 1
        later[found] = r
        return found + jnp.where((j > 0) & (d < slabs), 1, 0)

    found = lax.fori_loop(0, dest_ref.shape[0], number, 0, unroll=8)

    def send(i, started):
        r = later[i]
        d = dest_ref[r]
        p = lax.div(d, plane)
        e = filled[p]
        filled[p] = e + 1

        @pl.when(e < cap)
        def _():
            at = p * cap + e
            mark[at] = d - p * plane
            pltpu.make_async_copy(
                rows_ref.at[r], out_ref.at[at, :, pl.ds(0, features)], sem
            ).start()

        return started + jnp.where(e < cap, 1, 0)

    started = lax.fori_loop(0, found, send, 0)
    most = filled[0]
    for p in range(1, planes):
        most = jnp.maximum(most, filled[p])
    over = jnp.where(most > cap, 2 * plane, 0)

    def label(i, carry):
        value = (mark[i] + over).astype(jnp.float32)
        out_ref[i, :, pl.ds(features, 128)] = jnp.full((kinds, 128), value).astype(out_ref.dtype)
        return carry

    lax.fori_loop(0, places, label, 0)

    def finish(r, carry):
        pltpu.make_async_copy(rows_ref.at[0], out_ref.at[0, :, pl.ds(0, features)], sem).wait()
        return carry

    lax.fori_loop(0, started, finish, 0)


def spill(outlier_rows, destinations, outlier_counts, slab_count, planes):
    _, kinds, features = outlier_rows.shape
    smem = pl.BlockSpec(memory_space=pltpu.SMEM)
    plane = slab_count // planes
    return pl.pallas_call(
        lambda *refs: spill_kernel(plane, *refs),
        name="spill",
        in_specs=[smem, smem, pl.BlockSpec(memory_space=pl.ANY)],
        out_specs=pl.BlockSpec(memory_space=pltpu.VMEM),
        out_shape=jax.ShapeDtypeStruct((planes * SPILL, kinds, features + 128), outlier_rows.dtype),
        scratch_shapes=[
            pltpu.SMEM((slab_count + 1,), jnp.int32),
            pltpu.SMEM((outlier_rows.shape[0] + 1,), jnp.int32),
            pltpu.SMEM((planes,), jnp.int32),
            pltpu.SMEM((planes * SPILL,), jnp.int32),
            pltpu.SemaphoreType.DMA,
        ],
        cost_estimate=pl.CostEstimate(
            flops=2000000, bytes_accessed=4 * planes * SPILL * kinds * features, transcendentals=0
        ),
    )(destinations[:, 0], outlier_counts, outlier_rows)


def relay_kernel(here_ref, in_ref, *out_refs):
    places, kinds, width = in_ref.shape
    count = len(out_refs)
    senders = out_refs[0].shape[0] // kinds
    cap = places // senders
    total = places * kinds
    lanes = 128
    rows = in_ref[...].reshape(total, width)
    labels = rows[:, width - lanes :]
    corner = jnp.where(lax.broadcasted_iota(jnp.int32, (8, lanes), 1) == 0, 1.0, 0.0).astype(jnp.bfloat16)
    over = (((1,), (1,)), ((), ()))
    label = lax.dot_general(corner, labels, over, preferred_element_type=jnp.float32)[0:1]
    label = label.astype(jnp.int32)
    full = jnp.max(label, axis=1, keepdims=True) >= 2 * count
    owner = label & (2 * count - 1)
    x, y = here_ref[0], here_ref[1]
    ahead = (((owner >> 2) - x) & 3) * 4 + (((owner & 3) - y) & 3)
    ahead = jnp.where(owner < count, ahead, count)
    part = senders * kinds
    source = lax.broadcasted_iota(jnp.int32, (count * part, total), 1)
    target = lax.broadcasted_iota(jnp.int32, (count * part, total), 0)
    same = source % kinds == target % kinds
    same &= source // (cap * kinds) == target // kinds % senders
    picked = jnp.where(same & (ahead == target // part), 1.0, 0.0)
    some = jnp.max(picked, axis=1, keepdims=True) > 0.5
    picker = picked.astype(jnp.bfloat16)
    step = 512
    for c in range(0, width - lanes, step):
        got = jnp.dot(picker, rows[:, c : c + step], preferred_element_type=jnp.float32)
        got = jnp.where(some, got, EMPTY).astype(in_ref.dtype)
        for o in range(count):
            out_refs[o][:, c : c + step] = got[o * part : (o + 1) * part]
    told = jnp.where(full, 1.0, 0.0) * jnp.ones((part, lanes), jnp.float32)
    told = told.astype(in_ref.dtype)
    for o in range(count):
        out_refs[o][:, width - lanes :] = told


def relay(gathered, here, planes, count):
    _, kinds, width = gathered.shape
    return pl.pallas_call(
        relay_kernel,
        name="relay",
        in_specs=[pl.BlockSpec(memory_space=pltpu.SMEM), pl.BlockSpec(memory_space=pltpu.VMEM)],
        out_specs=[pl.BlockSpec(memory_space=pltpu.VMEM)] * count,
        out_shape=[jax.ShapeDtypeStruct((planes * kinds, width), gathered.dtype)] * count,
        cost_estimate=pl.CostEstimate(
            flops=10000000, bytes_accessed=4 * count * planes * kinds * width, transcendentals=0
        ),
    )(here, gathered)


def prepare_kernel(dirs_ref, order_ref, out_ref, rank_ref):
    tokens = dirs_ref.shape[1]
    for v in range(2):
        ahead = pltpu.roll(dirs_ref[v].astype(jnp.float32), tokens - 1, 0)
        out_ref[v] = ahead.astype(out_ref.dtype)

    @pl.when(pl.program_id(0) == 0)
    def _():
        token = lax.broadcasted_iota(jnp.int32, (tokens, tokens), 0)
        number = lax.broadcasted_iota(jnp.int32, (tokens, tokens), 1)
        here = jnp.where(order_ref[...] == token, number, 0).astype(jnp.float32)
        rank = jnp.sum(here, axis=1, keepdims=True).astype(jnp.int32)
        rank_ref[...] = jnp.broadcast_to(rank, rank_ref.shape)


def prepare(directions, order):
    _, tokens, features = directions.shape
    width = 256
    spec = pl.BlockSpec((2, tokens, width), lambda i: (0, 0, i))
    return pl.pallas_call(
        prepare_kernel,
        name="prepare",
        compiler_params=pltpu.CompilerParams(vmem_limit_bytes=16 * 2**20),
        grid=(features // width,),
        in_specs=[spec, pl.BlockSpec((1, tokens), lambda i: (0, 0))],
        out_specs=[spec, pl.BlockSpec((tokens, 128), lambda i: (0, 0))],
        out_shape=[
            jax.ShapeDtypeStruct(directions.shape, directions.dtype),
            jax.ShapeDtypeStruct((tokens, 128), jnp.int32),
        ],
        cost_estimate=pl.CostEstimate(
            flops=20 * tokens * features, bytes_accessed=8 * tokens * features, transcendentals=0
        ),
    )(directions, order)


def place_kernel(
    pieces, first, order, rank, dirs, mags, edge, *rest_of
):
    second, rest_of = rest_of[:pieces], rest_of[pieces:]
    (
    out,
    a_buf, b_buf, k_buf, r_buf, d_buf, m_buf, e_buf, o_buf, placer, covered, wide,
    a_sem, k_sem, r_sem, d_sem, m_sem, e_sem, o_sem,
) = rest_of
    blocks, kinds, tokens, width = o_buf.shape
    half = a_buf.shape[1]
    slots = 2 * half
    lanes = 128
    chunks = slots // lanes
    heads = width // lanes

    def columns(i):
        return pl.ds(pl.multiple_of(i * width, lanes), width)

    class a_copy:
        def __init__(self, i):
            size = b_buf.shape[1] // pieces
            self.parts = [
                pltpu.make_async_copy(first.at[:, :, columns(i)], a_buf.at[i], a_sem.at[i, 0])
            ] + [
                pltpu.make_async_copy(
                    piece.at[:, columns(i)], b_buf.at[i, pl.ds(o * size, size)], a_sem.at[i, 1]
                )
                for o, piece in enumerate(second)
            ]
            self.whole = pltpu.make_async_copy(b_buf.at[i], b_buf.at[i], a_sem.at[i, 1])

        def start(self):
            for part in self.parts:
                part.start()

        def wait(self):
            self.parts[0].wait()
            self.whole.wait()

    def d_copy(i):
        return pltpu.make_async_copy(dirs.at[:, :, columns(i)], d_buf.at[i], d_sem.at[i])

    def o_copy(i):
        return pltpu.make_async_copy(o_buf.at[i], out.at[:, :, columns(i)], o_sem.at[i])

    r_copy = pltpu.make_async_copy(rank, r_buf, r_sem)
    k_copy = pltpu.make_async_copy(order, k_buf, k_sem)
    m_copy = pltpu.make_async_copy(mags, m_buf, m_sem)
    e_copy = pltpu.make_async_copy(edge, e_buf, e_sem)
    a_copy(0).start()
    k_copy.start()
    r_copy.start()
    m_copy.start()
    e_copy.start()
    d_copy(0).start()
    for i in range(1, DEPTH):
        a_copy(i).start()
        d_copy(i).start()


    def block(i, carry):
        @pl.when(i + DEPTH < blocks)
        def _():
            a_copy(i + DEPTH).start()
            d_copy(i + DEPTH).start()

        a_copy(i).wait()
        for c in range(heads):
            part = slice(c * lanes, (c + 1) * lanes)
            wide[c, : half * kinds] = (
                a_buf[i, :, :, part].reshape(half * kinds, lanes).astype(jnp.float32)
            )
            wide[c, half * kinds :] = b_buf[i, :, part].astype(jnp.float32)

        @pl.when(i == 0)
        def _():
            corner_of = wide[0, pl.ds(0, slots, stride=kinds), :]
            full = jnp.where(corner_of < EMPTY, 1.0, 0.0).astype(jnp.bfloat16)
            corner = jnp.where(lax.broadcasted_iota(jnp.int32, (8, lanes), 1) == 0, 1.0, 0.0)
            corner = corner.astype(jnp.bfloat16)
            over = (((1,), (1,)), ((), ()))
            filled = [
                lax.dot_general(
                    corner, full[c * lanes : (c + 1) * lanes], over, preferred_element_type=jnp.float32
                )
                for c in range(chunks)
            ]
            run = jnp.sum(sum(filled), axis=1, keepdims=True)[0:1]
            k_copy.wait()
            ahead = []
            for c in range(chunks):
                number = jnp.zeros((8, lanes), jnp.float32)
                for e in range(chunks):
                    earlier = k_buf[e, :, :] < k_buf[2 + c, 0:1, :]
                    number += jnp.dot(
                        filled[e].astype(jnp.bfloat16),
                        jnp.where(earlier, 1.0, 0.0).astype(jnp.bfloat16),
                        preferred_element_type=jnp.float32,
                    )
                ahead.append(jnp.where(filled[c] > 0.5, number, -1.0).astype(jnp.int32))
            r_copy.wait()
            m_copy.wait()
            e_copy.wait()
            place_of = r_buf[...]
            covered[...] = jnp.where(place_of < run.astype(jnp.int32), 1, 0)
            for c in range(chunks):
                placer[:, c * lanes : (c + 1) * lanes] = jnp.where(
                    place_of == ahead[c][0:1], 1.0, 0.0
                ).astype(jnp.bfloat16)

        d_copy(i).wait()
        tail = slice(tokens - 16, tokens)
        last = lax.broadcasted_iota(jnp.int32, (16, width), 0) == 15
        for v in range(2):
            end = d_buf[i, v, tail].astype(jnp.float32)
            end = jnp.where(last, e_buf[v : v + 1, columns(i)], end)
            d_buf[i, v, tail] = end.astype(d_buf.dtype)
        given = e_buf[2:3, pl.ds(pl.multiple_of(i * lanes, lanes), lanes)]
        m_buf[i, tail] = jnp.where(last[:, 0:lanes], given, m_buf[i, tail])
        factors = jnp.where(covered[...] > 0, 0.0, m_buf[i])
        own_dirs = [d_buf[i, v].astype(jnp.float32) for v in range(2)]
        for k in range(kinds):
          for c0 in range(0, heads, 2):
            rows = jnp.concatenate(
                [wide[c, pl.ds(k, slots, stride=kinds), :] for c in range(c0, c0 + 2)], axis=1
            ).astype(jnp.bfloat16)
            both = jnp.dot(placer[...], rows, preferred_element_type=jnp.float32)
            for c in range(c0, c0 + 2):
                part = slice(c * lanes, (c + 1) * lanes)
                got = both[:, (c - c0) * lanes : (c - c0 + 1) * lanes]
                own = factors[:, k * heads + c : k * heads + c + 1] * own_dirs[k % 2][:, part]
                o_buf[i, k, :, part] = (got + own).astype(o_buf.dtype)
        o_copy(i).start()
        return carry

    lax.fori_loop(0, blocks, block, 0)
    for i in range(blocks):
        o_copy(i).wait()


def place(first, second, order, rank, dirs, mags, edge):
    slabs, kinds, features = first.shape
    slots = 2 * slabs
    _, tokens, _ = dirs.shape
    width = WIDTH
    blocks = features // width
    anywhere = pl.BlockSpec(memory_space=pl.ANY)
    return pl.pallas_call(
        functools.partial(place_kernel, len(second)),
        name="place",
        in_specs=[anywhere] * (6 + len(second)),
        out_specs=anywhere,
        out_shape=jax.ShapeDtypeStruct((kinds, tokens, features), first.dtype),
        scratch_shapes=[
            pltpu.VMEM((blocks, slabs, kinds, width), first.dtype),
            pltpu.VMEM((blocks, slabs * kinds, width), first.dtype),
            pltpu.VMEM(order.shape, order.dtype),
            pltpu.VMEM(rank.shape, rank.dtype),
            pltpu.VMEM((blocks, 2, tokens, width), dirs.dtype),
            pltpu.VMEM(mags.shape, mags.dtype),
            pltpu.VMEM(edge.shape, edge.dtype),
            pltpu.VMEM((blocks, kinds, tokens, width), first.dtype),
            pltpu.VMEM((tokens, slots), jnp.bfloat16),
            pltpu.VMEM((tokens, 128), jnp.int32),
            pltpu.VMEM((width // 128, slots * kinds, 128), jnp.float32),
            pltpu.SemaphoreType.DMA((blocks, 2)),
            pltpu.SemaphoreType.DMA,
            pltpu.SemaphoreType.DMA,
            pltpu.SemaphoreType.DMA((blocks,)),
            pltpu.SemaphoreType.DMA,
            pltpu.SemaphoreType.DMA,
            pltpu.SemaphoreType.DMA((blocks,)),
        ],
        cost_estimate=pl.CostEstimate(
            flops=2 * kinds * tokens * slots * features,
            bytes_accessed=2 * (slots * kinds + 2 * tokens + kinds * tokens) * features,
            transcendentals=0,
        ),
    )(first, order, rank, dirs, mags, edge, *second)


def passed_back(block, axis):
    devices = lax.axis_size(axis)
    return lax.ppermute(block, axis, [((i + 1) % devices, i) for i in range(devices)])


def per_device(directions, magnitudes, outlier_rows, outlier_counts, destinations, retention_order):
    slab_count = lax.axis_size(SLAB)
    features = directions.shape[2]
    heads = magnitudes.shape[1]
    planes = lax.axis_size("slab_0")
    plane = ("slab_1", "slab_2")
    wide, deep = lax.axis_size("slab_1"), lax.axis_size("slab_2")
    x, y = lax.axis_index("slab_1"), lax.axis_index("slab_2")

    spilled = spill(outlier_rows, destinations, outlier_counts, slab_count, planes)
    gathered = lax.all_to_all(spilled, "slab_0", split_axis=0, concat_axis=0, tiled=True)
    packed = pack(outlier_rows, destinations, outlier_counts, slab_count, 0)
    packed, gathered = lax.optimization_barrier((packed, gathered))
    first = lax.all_to_all(packed, SLAB, split_axis=0, concat_axis=0, tiled=True)

    sorted_rows = relay(gathered, jnp.stack([x, y]).astype(jnp.int32), planes, wide * deep)
    steps = [(dx, dy) for dx in range(wide) for dy in range(deep)]
    second = []
    for (dx, dy), rows in zip(steps, sorted_rows):
        if (dx, dy) != (0, 0):
            route = [
                (i * deep + j, (i + dx) % wide * deep + (j + dy) % deep)
                for i in range(wide)
                for j in range(deep)
            ]
            rows = lax.ppermute(rows, plane, route)
        second.append(rows)
    told = functools.reduce(jnp.maximum, [rows[:, features:] for rows in second])
    too_many = jnp.max(told) > 0.5

    slabs = jnp.arange(slab_count, dtype=jnp.int32)
    step, z = slabs // planes, slabs % planes
    came = z * (wide * deep) + (x - step // deep) % wide * deep + (y - step % deep) % deep

    def order_of(first_slab, second_slab):
        keys = jnp.stack([2 * first_slab, 2 * second_slab + 1]).astype(jnp.int32)
        return jnp.concatenate(
            [
                jnp.broadcast_to(keys[:, :, None], (2, slab_count, 128)),
                jnp.broadcast_to(keys[:, None, :], (2, slab_count, 128)),
            ]
        )

    blocks = features // WIDTH

    def by_block(block):
        count = block.shape[2]
        block = block.reshape(4, blocks, heads // blocks, count).transpose(1, 3, 0, 2)
        block = block.reshape(blocks, count, 4 * heads // blocks)
        return jnp.pad(block, ((0, 0), (0, 0), (0, 128 - block.shape[2])))

    first_mags = by_block(magnitudes[:, :, :1]).reshape(1, blocks * 128)
    edge = jnp.concatenate(
        [
            directions[:, 0, :].astype(jnp.float32),
            jnp.pad(first_mags, ((0, 1), (0, features - blocks * 128))),
        ]
    )
    edge = passed_back(edge, SLAB)
    factors = by_block(jnp.roll(magnitudes, -1, axis=2))
    factors = with_layout_constraint(factors, Layout(major_to_minor=(0, 1, 2)))
    dirs, rank = prepare(directions, retention_order)
    relayed, direct = order_of(slabs, came), order_of(slabs, slabs)

    def short(_):
        return place(first, second, relayed, rank, dirs, factors, edge)

    def long(_):
        rest = pack(outlier_rows, destinations, outlier_counts, slab_count, 1)
        rest = lax.all_to_all(rest, SLAB, split_axis=0, concat_axis=0, tiled=True)
        rest = jnp.split(rest.reshape(-1, features), len(second))
        return place(first, rest, direct, rank, dirs, factors, edge)

    return lax.cond(too_many, long, short, 0)


def solution(mesh):
    finer = Mesh(
        mesh.devices.reshape(8, 4, 4, mesh.shape["head"]), ("slab_0", "slab_1", "slab_2", "head")
    )
    placed = (
        P(None, SLAB, "head"),
        P(None, "head", SLAB),
        P(SLAB, None, "head"),
        P(SLAB),
        P(SLAB, None),
        P(SLAB, None),
    )
    return jax.shard_map(
        per_device, mesh=finer, in_specs=placed, out_specs=P(None, SLAB, "head"), check_vma=False
    )
```
